32 devices in a mesh: data: 1 (over z), model: 32 (over y, x, core).
Axes of the slice: x: 4, y: 4, z: 1, core: 2. Of those that a mesh axis runs over, the one named last changes fastest.
The devices are a block of a 4x4x8 slice.
Arguments:
- x_in: bfloat16 [4096, 4096], P(('data', 'model'))
- dy_in: bfloat16 [4096, 4096], P(('data', 'model'))
- w_query: bfloat16 [4096, 32, 128], P(None, 'model')
- w_key: bfloat16 [4096, 128], replicated
- w_value: bfloat16 [4096, 128], replicated
- w_out: bfloat16 [32, 128, 4096], P('model')
Outputs:
- output 1: bfloat16 [4096, 4096], P(('data', 'model'))
- output 2: float32 [4096, 32, 128], P('data', 'model')
- output 3: float32 [4096, 128], P(('data', 'model'))
- output 4: float32 [4096, 128], P(('data', 'model'))
- output 5: float32 [32, 128, 4096], P(('data', 'model'))
All inputs are finite; a program needn't handle non-finite values.
Results may differ from the reference program's by a relative error of at most 0.00898.
Values are sent between devices in bfloat16 or wider.
A program may use at most 768 MiB of HBM per device.

```python
import math
import jax
import jax.numpy as jnp
from jax import lax

SEQ_LEN = 4096
D_MODEL = 4096
NUM_HEADS = 32
HEAD_DIM = 128


def setup_inputs(seed: int = 0, part: int = 0) -> dict:
    part_key = jax.random.fold_in(jax.random.key(seed), part)
    act_keys = jax.random.split(part_key, 2)
    weight_keys = jax.random.split(jax.random.key(seed + 1), 4)
    in_scale = D_MODEL ** -0.5
    x_in = jax.random.normal(act_keys[0], (SEQ_LEN, D_MODEL), jnp.float32).astype(jnp.bfloat16)
    dy_in = jax.random.normal(act_keys[1], (SEQ_LEN, D_MODEL), jnp.float32).astype(jnp.bfloat16)
    w_query = (jax.random.normal(weight_keys[0], (D_MODEL, NUM_HEADS, HEAD_DIM), jnp.float32) * in_scale).astype(jnp.bfloat16)
    w_key = (jax.random.normal(weight_keys[1], (D_MODEL, HEAD_DIM), jnp.float32) * in_scale).astype(jnp.bfloat16)
    w_value = (jax.random.normal(weight_keys[2], (D_MODEL, HEAD_DIM), jnp.float32) * in_scale).astype(jnp.bfloat16)
    w_out = (jax.random.normal(weight_keys[3], (NUM_HEADS, HEAD_DIM, D_MODEL), jnp.float32) * in_scale).astype(jnp.bfloat16)
    return {"x_in": x_in, "dy_in": dy_in, "w_query": w_query, "w_key": w_key, "w_value": w_value, "w_out": w_out}


def reference(x_in, dy_in, w_query, w_key, w_value, w_out):
    score_scale = 1.0 / math.sqrt(HEAD_DIM)
    keys_all = jnp.dot(x_in, w_key, preferred_element_type=jnp.float32).astype(jnp.bfloat16)
    values_all = jnp.dot(x_in, w_value, preferred_element_type=jnp.float32).astype(jnp.bfloat16)
    causal = jnp.arange(SEQ_LEN)[:, None] >= jnp.arange(SEQ_LEN)[None, :]

    def head_step(carry_in, head_weights):
        dk_sum, dv_sum, dx_sum = carry_in
        wq_head, wo_head = head_weights
        query_rows = jnp.dot(x_in, wq_head, preferred_element_type=jnp.float32).astype(jnp.bfloat16)
        scores = jnp.dot(query_rows, keys_all.T, preferred_element_type=jnp.float32) * score_scale
        scores = jnp.where(causal, scores, -jnp.inf)
        probs_f32 = jax.nn.softmax(scores, axis=-1)
        probs_bf = probs_f32.astype(jnp.bfloat16)
        attn_rows = jnp.dot(probs_bf, values_all, preferred_element_type=jnp.float32).astype(jnp.bfloat16)
        dw_out_head = jnp.dot(attn_rows.T, dy_in, preferred_element_type=jnp.float32)
        d_attn = jnp.dot(dy_in, wo_head.T, preferred_element_type=jnp.float32).astype(jnp.bfloat16)
        d_probs = jnp.dot(d_attn, values_all.T, preferred_element_type=jnp.float32)
        row_dot = jnp.sum(d_attn.astype(jnp.float32) * attn_rows.astype(jnp.float32), axis=-1, keepdims=True)
        d_scores = (probs_f32 * (d_probs - row_dot) * score_scale).astype(jnp.bfloat16)
        d_query = jnp.dot(d_scores, keys_all, preferred_element_type=jnp.float32).astype(jnp.bfloat16)
        d_keys_part = jnp.dot(d_scores.T, query_rows, preferred_element_type=jnp.float32)
        d_values_part = jnp.dot(probs_bf.T, d_attn, preferred_element_type=jnp.float32)
        dw_query_head = jnp.dot(x_in.T, d_query, preferred_element_type=jnp.float32)
        dx_part = jnp.dot(d_query, wq_head.T, preferred_element_type=jnp.float32)
        carry_out = (dk_sum + d_keys_part, dv_sum + d_values_part, dx_sum + dx_part)
        return carry_out, (dw_query_head, dw_out_head)

    carry_init = (jnp.zeros((SEQ_LEN, HEAD_DIM), jnp.float32), jnp.zeros((SEQ_LEN, HEAD_DIM), jnp.float32), jnp.zeros((SEQ_LEN, D_MODEL), jnp.float32))
    wq_heads = jnp.transpose(w_query, (1, 0, 2))
    sums_out, grads_out = lax.scan(head_step, carry_init, (wq_heads, w_out))
    dk_sum, dv_sum, dx_sum = sums_out
    dwq_heads, dw_out = grads_out
    d_keys = dk_sum.astype(jnp.bfloat16)
    d_values = dv_sum.astype(jnp.bfloat16)
    dw_key = jnp.dot(x_in.T, d_keys, preferred_element_type=jnp.float32)
    dw_value = jnp.dot(x_in.T, d_values, preferred_element_type=jnp.float32)
    dx_total = dx_sum + jnp.dot(d_keys, w_key.T, preferred_element_type=jnp.float32) + jnp.dot(d_values, w_value.T, preferred_element_type=jnp.float32)
    dx_out = dx_total.astype(jnp.bfloat16)
    dw_query = jnp.transpose(dwq_heads, (1, 0, 2))
    return (dx_out, dw_query, dw_key, dw_value, dw_out)
```

```python
import functools
import math
import jax
import jax.numpy as jnp
from jax import lax
from jax.experimental import pallas as pl
from jax.experimental.pallas import tpu as pltpu
from jax.sharding import PartitionSpec as P

BLK = 512
F32 = jnp.float32
BF16 = jnp.bfloat16


def _dot(a, b):
    return jnp.dot(a, b, preferred_element_type=F32)


def _flip(a):
    return jnp.transpose(a.astype(F32))


def _fwd_kernel(scale, q_ref, k_ref, vt_ref, o_ref, st_ref, s_ref):
    i = pl.program_id(0)
    qt = _flip(q_ref[...]).astype(BF16)

    def score(j, m8, diag):
        s = _dot(k_ref[pl.ds(pl.multiple_of(j * BLK, BLK), BLK), :], qt) * scale
        if diag:
            key = lax.broadcasted_iota(jnp.int32, (BLK, BLK), 0)
            qry = lax.broadcasted_iota(jnp.int32, (BLK, BLK), 1)
            s = jnp.where(qry >= key, s, -jnp.inf)
        s_ref[j] = s
        return jnp.maximum(m8, jnp.max(s.reshape(BLK // 8, 8, BLK), axis=0))

    m8 = jnp.full((8, BLK), -jnp.inf, F32)
    m8 = lax.fori_loop(0, i, lambda j, c: score(j, c, False), m8)
    m8 = score(i, m8, True)
    m = jnp.max(m8, axis=0, keepdims=True)

    def expo(j, l8):
        p = jnp.exp(s_ref[j] - m)
        s_ref[j] = p
        return l8 + jnp.sum(p.reshape(BLK // 8, 8, BLK), axis=0)

    l8 = lax.fori_loop(0, i + 1, expo, jnp.zeros((8, BLK), F32))
    r = 1.0 / jnp.sum(l8, axis=0, keepdims=True)

    def attend(j, ot):
        return ot + _dot(vt_ref[j], (s_ref[j] * r).astype(BF16))

    ot = lax.fori_loop(0, i + 1, attend, jnp.zeros((o_ref.shape[1], BLK), F32))
    o_ref[...] = jnp.transpose(ot).astype(BF16)
    row = lax.broadcasted_iota(jnp.int32, (8, BLK), 0)
    st_ref[...] = jnp.where(row == 0, m, r)


def _bwd_kernel(scale, q_ref, do_ref, o_ref, st_ref, k_ref, v_ref, kt_ref, dq_ref, dkv_ref):
    i = pl.program_id(0)
    hd = q_ref.shape[1]

    @pl.when(i == 0)
    def _():
        dkv_ref[...] = jnp.zeros_like(dkv_ref)

    qt = _flip(q_ref[...]).astype(BF16)
    dot_f = _flip(do_ref[...])
    c = jnp.sum(dot_f * _flip(o_ref[...]), axis=0, keepdims=True)
    dot_b = dot_f.astype(BF16)
    m = st_ref[0:1, :]
    r = st_ref[1:2, :]

    def step(j, dqt, diag):
        rows = pl.ds(pl.multiple_of(j * BLK, BLK), BLK)
        s = _dot(k_ref[rows, :], qt) * scale
        if diag:
            key = lax.broadcasted_iota(jnp.int32, (BLK, BLK), 0)
            qry = lax.broadcasted_iota(jnp.int32, (BLK, BLK), 1)
            s = jnp.where(qry >= key, s, -jnp.inf)
        p = jnp.exp(s - m) * r
        dp = _dot(v_ref[rows, :], dot_b)
        g = (p * (dp - c) * scale).astype(BF16)
        dkv_ref[rows, 0:hd] += _dot(g, q_ref[...])
        dkv_ref[rows, hd : 2 * hd] += _dot(p.astype(BF16), do_ref[...])
        return dqt + _dot(kt_ref[j], g)

    dqt = jnp.zeros((hd, BLK), F32)
    dqt = lax.fori_loop(0, i, lambda j, a: step(j, a, False), dqt)
    dqt = step(i, dqt, True)
    dq_ref[...] = jnp.transpose(dqt).astype(BF16)


def _attn_fwd(q, k, vt, scale):
    t, hd = q.shape
    n = t // BLK
    return pl.pallas_call(
        functools.partial(_fwd_kernel, scale),
        grid=(n,),
        in_specs=[
            pl.BlockSpec((BLK, hd), lambda i: (i, 0)),
            pl.BlockSpec((t, hd), lambda i: (0, 0)),
            pl.BlockSpec((n, hd, BLK), lambda i: (0, 0, 0)),
        ],
        out_specs=[pl.BlockSpec((BLK, hd), lambda i: (i, 0)), pl.BlockSpec((8, BLK), lambda i: (0, i))],
        out_shape=[jax.ShapeDtypeStruct((t, hd), BF16), jax.ShapeDtypeStruct((8, t), F32)],
        scratch_shapes=[pltpu.VMEM((n, BLK, BLK), F32)],
        compiler_params=pltpu.CompilerParams(vmem_limit_bytes=40 * 2**20),
        cost_estimate=pl.CostEstimate(flops=40 * 10**9, bytes_accessed=8 * t * hd, transcendentals=t * t // 2),
        name="attn_fwd",
    )(q, k, vt)


def _attn_bwd(q, do, o, st, k, v, kt, scale):
    t, hd = q.shape
    n = t // BLK
    blk = pl.BlockSpec((BLK, hd), lambda i: (i, 0))
    whole = pl.BlockSpec((t, hd), lambda i: (0, 0))
    return pl.pallas_call(
        functools.partial(_bwd_kernel, scale),
        grid=(n,),
        in_specs=[
            blk, blk, blk,
            pl.BlockSpec((8, BLK), lambda i: (0, i)),
            whole, whole,
            pl.BlockSpec((n, hd, BLK), lambda i: (0, 0, 0)),
        ],
        out_specs=[blk, pl.BlockSpec((t, 2 * hd), lambda i: (0, 0))],
        out_shape=[jax.ShapeDtypeStruct((t, hd), BF16), jax.ShapeDtypeStruct((t, 2 * hd), F32)],
        compiler_params=pltpu.CompilerParams(vmem_limit_bytes=40 * 2**20),
        cost_estimate=pl.CostEstimate(flops=60 * 10**9, bytes_accessed=16 * t * hd, transcendentals=t * t // 2),
        name="attn_bwd",
    )(q, do, o, st, k, v, kt)


def _tail_kernel(n, dq_ref, dkv_ref, dqa_ref, all_ref, pbuf, sbuf, rbuf, q_sem, p_sem, r_sem, g_sem, f_sem, e_sem, l_sem):
    me = lax.axis_index("model")
    core = lax.rem(me, 2)
    chip = me // 2
    nc = n // 2
    other = 1 - core
    partner = me + 1 - 2 * core
    blk = dkv_ref.shape[2]

    def dev(idx):
        return {"model": idx}

    barrier = pltpu.get_barrier_semaphore()

    @pl.loop(1, n)
    def _(o):
        pl.semaphore_signal(barrier, inc=1, device_id=dev(lax.rem(me + o, n)), device_id_type=pl.DeviceIdType.MESH)

    pl.semaphore_wait(barrier, n - 1)

    pair = pltpu.make_async_remote_copy(
        dkv_ref.at[:, other], pbuf, p_sem.at[0], p_sem.at[1], device_id=dev(partner), device_id_type=pl.DeviceIdType.MESH)
    pair.start()

    def q_copy(o):
        peer = lax.rem(me + o, n)
        return pltpu.make_async_remote_copy(
            dq_ref.at[peer], dqa_ref.at[me], q_sem.at[0, o], q_sem.at[1, o], device_id=dev(peer), device_id_type=pl.DeviceIdType.MESH)

    @pl.loop(1, n)
    def _(o):
        q_copy(o).start()

    mine = pltpu.make_async_copy(dq_ref.at[me], dqa_ref.at[me], l_sem)
    mine.start()
    pair.wait()

    def r_copy(o):
        peer = lax.rem(chip + o, nc) * 2 + core
        return pltpu.make_async_remote_copy(
            sbuf.at[o], rbuf.at[o], r_sem.at[0, o], r_sem.at[1, o], device_id=dev(peer), device_id_type=pl.DeviceIdType.MESH)

    @pl.loop(1, nc)
    def _(o):
        t = lax.rem(chip + o, nc)
        sbuf[o] = dkv_ref[t, core] + pbuf[t]
        r_copy(o).start()

    rbuf[0] = dkv_ref[chip, core] + pbuf[chip]

    @pl.loop(1, nc)
    def _(o):
        r_copy(o).wait()
        rbuf[0] += rbuf[o]

    all_ref[me] = rbuf[0].astype(BF16)

    def g_copy(o):
        peer = lax.rem(chip + o, nc) * 2 + core
        return pltpu.make_async_remote_copy(
            all_ref.at[me], all_ref.at[me], g_sem.at[0, o], g_sem.at[1, o], device_id=dev(peer), device_id_type=pl.DeviceIdType.MESH)

    def f_copy(o):
        src = lax.rem(chip + nc - o, nc) * 2 + core
        return pltpu.make_async_remote_copy(
            all_ref.at[src], all_ref.at[src], f_sem.at[0, o], f_sem.at[1, o], device_id=dev(partner), device_id_type=pl.DeviceIdType.MESH)

    own = pltpu.make_async_remote_copy(
        all_ref.at[me], all_ref.at[me], e_sem.at[0], e_sem.at[1], device_id=dev(partner), device_id_type=pl.DeviceIdType.MESH)

    @pl.loop(1, nc)
    def _(o):
        g_copy(o).start()

    own.start()

    @pl.loop(1, nc)
    def _(o):
        g_copy(o).wait()
        f_copy(o).start()

    own.wait()
    mine.wait()

    @pl.loop(1, nc)
    def _(o):
        f_copy(o).wait()

    @pl.loop(1, n)
    def _(o):
        q_copy(o).wait()


def _tail(dq, dkv, n):
    t, hd = dq.shape
    b = t // n
    nc = n // 2
    vmem = pl.BlockSpec(memory_space=pltpu.VMEM)
    dma = pltpu.SemaphoreType.DMA
    return pl.pallas_call(
        functools.partial(_tail_kernel, n),
        in_specs=[vmem, vmem],
        out_specs=[vmem, vmem],
        out_shape=[jax.ShapeDtypeStruct((n, b, hd), BF16), jax.ShapeDtypeStruct((n, b, 2 * hd), BF16)],
        scratch_shapes=[
            pltpu.VMEM((nc, b, 2 * hd), F32),
            pltpu.VMEM((nc, b, 2 * hd), F32),
            pltpu.VMEM((nc, b, 2 * hd), F32),
            dma((2, n)), dma((2,)), dma((2, nc)), dma((2, nc)), dma((2, nc)), dma((2,)), dma,
        ],
        compiler_params=pltpu.CompilerParams(collective_id=1, has_side_effects=True, vmem_limit_bytes=32 * 2**20),
        cost_estimate=pl.CostEstimate(flops=30 * 10**9, bytes_accessed=16 * t * hd, transcendentals=0),
        name="tail_exchange",
    )(dq.reshape(n, b, hd), dkv.reshape(nc, 2, b, 2 * hd))


def _dx_kernel(nh, dqa_ref, own_ref, wq_ref, wk_ref, wv_ref, dx_ref):
    dims = (((1,), (1,)), ((), ()))

    def term(a0, a1, w0, w1):
        a = jnp.concatenate([a0, a1], axis=1)
        w = jnp.concatenate([w0, w1], axis=1)
        return lax.dot_general(a, w, dims, preferred_element_type=F32)

    hd = wk_ref.shape[1]
    acc = term(own_ref[:, 0:hd], own_ref[:, hd : 2 * hd], wk_ref[...], wv_ref[...])
    for h in range(0, nh, 2):
        acc = acc + term(dqa_ref[h], dqa_ref[h + 1], wq_ref[h], wq_ref[h + 1])
    dx_ref[...] = acc.astype(BF16)


def _dx(dqa, own, wq_all, w_key, w_value):
    nh, b, hd = dqa.shape
    d = w_key.shape[0]
    dt = 512
    return pl.pallas_call(
        functools.partial(_dx_kernel, nh),
        grid=(d // dt,),
        in_specs=[
            pl.BlockSpec((nh, b, hd), lambda i: (0, 0, 0)),
            pl.BlockSpec((b, 2 * hd), lambda i: (0, 0)),
            pl.BlockSpec((nh, dt, hd), lambda i: (0, i, 0)),
            pl.BlockSpec((dt, hd), lambda i: (i, 0)),
            pl.BlockSpec((dt, hd), lambda i: (i, 0)),
        ],
        out_specs=pl.BlockSpec((b, dt), lambda i: (0, i)),
        out_shape=jax.ShapeDtypeStruct((b, d), BF16),
        compiler_params=pltpu.CompilerParams(vmem_limit_bytes=32 * 2**20),
        cost_estimate=pl.CostEstimate(flops=2 * nh * b * d * hd, bytes_accessed=2 * nh * d * hd, transcendentals=0),
        name="dx_rows",
    )(dqa, own, wq_all, w_key, w_value)


def solution(mesh):
    tok_spec = P(("data", "model"), None)
    n = mesh.shape["model"]

    def local_step(x_loc, dy_loc, wq_loc, w_key, w_value, wo_loc):
        d, hd = w_key.shape
        scale = 1.0 / math.sqrt(hd)
        wq_h = wq_loc.reshape(d, hd)
        x_full = lax.all_gather(x_loc, "model", axis=0, tiled=True)
        dy_full = lax.all_gather(dy_loc, "model", axis=0, tiled=True)
        wq_all = lax.all_gather(wq_h, "model", axis=0, tiled=True).reshape(n, d, hd)
        t = x_full.shape[0]
        nb = t // BLK
        w3 = jnp.concatenate([wq_h, w_key, w_value], axis=1)
        qkv = jnp.dot(x_full, w3, preferred_element_type=F32).astype(BF16)
        q, k, v = qkv[:, :hd], qkv[:, hd : 2 * hd], qkv[:, 2 * hd :]
        vt = v.reshape(nb, BLK, hd).transpose(0, 2, 1)
        kt = k.reshape(nb, BLK, hd).transpose(0, 2, 1)
        o, st = _attn_fwd(q, k, vt, scale)
        o, dy_full = lax.optimization_barrier((o, dy_full))
        d_attn = jnp.einsum("td,ed->te", dy_full, wo_loc.reshape(hd, d), preferred_element_type=F32).astype(BF16)
        dq, dkv = _attn_bwd(q, d_attn, o, st, k, v, kt, scale)
        dw_out = jnp.einsum("te,td->ed", o, dy_full, preferred_element_type=F32)[None]
        dw_query = jnp.einsum("td,te->de", x_full, dq, preferred_element_type=F32)[:, None, :]
        dq, dkv, dw_query, dw_out = lax.optimization_barrier((dq, dkv, dw_query, dw_out))
        dqa, dkv_all = _tail(dq, dkv, n)
        me = lax.axis_index("model")
        own = lax.dynamic_index_in_dim(dkv_all, me, 0, keepdims=False)
        dx = _dx(dqa, own, wq_all, w_key, w_value)
        cols = lax.dynamic_slice_in_dim(x_full, me * (d // n), d // n, axis=1)
        dwkv = jnp.einsum("td,te->de", cols, dkv_all.reshape(t, 2 * hd), preferred_element_type=F32)
        return (dx, dw_query, dwkv[:, :hd], dwkv[:, hd:], dw_out)

    return jax.shard_map(
        local_step, mesh=mesh,
        in_specs=(tok_spec, tok_spec, P(None, "model", None), P(None, None), P(None, None), P("model", None, None)),
        out_specs=(tok_spec, P("data", "model", None), tok_spec, tok_spec, P(("data", "model"), None, None)),
        check_vma=False)
```

```python
import functools
import math
import jax
import jax.numpy as jnp
from jax import lax
from jax.experimental import pallas as pl
from jax.experimental.pallas import tpu as pltpu
from jax.sharding import PartitionSpec as P

BLK = 512
F32 = jnp.float32
BF16 = jnp.bfloat16
MESH_ID = pl.DeviceIdType.MESH


def _dot(a, b):
    return jnp.dot(a, b, preferred_element_type=F32)


def _flip(a):
    return jnp.transpose(a.astype(F32))


def _fwd_block(scale, i, q_ref, k_ref, vt_ref, ot_ref, st_ref, s_ref):
    here = pl.ds(pl.multiple_of(i * BLK, BLK), BLK)
    qt = _flip(q_ref[here, :]).astype(BF16)

    def score(j, m8, diag):
        s = _dot(k_ref[pl.ds(pl.multiple_of(j * BLK, BLK), BLK), :], qt) * scale
        if diag:
            key = lax.broadcasted_iota(jnp.int32, (BLK, BLK), 0)
            qry = lax.broadcasted_iota(jnp.int32, (BLK, BLK), 1)
            s = jnp.where(qry >= key, s, -jnp.inf)
        s_ref[j] = s
        return jnp.maximum(m8, jnp.max(s.reshape(BLK // 8, 8, BLK), axis=0))

    m8 = jnp.full((8, BLK), -jnp.inf, F32)
    m8 = lax.fori_loop(0, i, lambda j, c: score(j, c, False), m8)
    m8 = score(i, m8, True)
    m = jnp.max(m8, axis=0, keepdims=True)

    def expo(j, l8):
        p = jnp.exp(s_ref[j] - m)
        s_ref[j] = p
        return l8 + jnp.sum(p.reshape(BLK // 8, 8, BLK), axis=0)

    l8 = lax.fori_loop(0, i + 1, expo, jnp.zeros((8, BLK), F32))
    r = 1.0 / jnp.sum(l8, axis=0, keepdims=True)

    def attend(j, ot):
        return ot + _dot(vt_ref[j], (s_ref[j] * r).astype(BF16))

    ot = lax.fori_loop(0, i + 1, attend, jnp.zeros(ot_ref.shape[1:], F32))
    ot_ref[i] = ot.astype(BF16)
    row = lax.broadcasted_iota(jnp.int32, (8, BLK), 0)
    st_ref[i] = jnp.where(row == 0, m, r)


def _bwd_block(scale, i, q_ref, do_ref, ot_ref, st_ref, k_ref, v_ref, kt_ref, dq_ref, dqt_ref, dkv_ref):
    here = pl.ds(pl.multiple_of(i * BLK, BLK), BLK)
    hd = q_ref.shape[1]
    qt = _flip(q_ref[here, :]).astype(BF16)
    dot_f = _flip(do_ref[here, :])
    c = jnp.sum(dot_f * ot_ref[i].astype(F32), axis=0, keepdims=True)
    dot_b = dot_f.astype(BF16)
    m = st_ref[i, 0:1, :]
    r = st_ref[i, 1:2, :]
    chips = BLK // (dkv_ref.shape[1] * dkv_ref.shape[2])

    def step(j, dqt, diag):
        rows = pl.ds(pl.multiple_of(j * BLK, BLK), BLK)
        s = _dot(k_ref[rows, :], qt) * scale
        if diag:
            key = lax.broadcasted_iota(jnp.int32, (BLK, BLK), 0)
            qry = lax.broadcasted_iota(jnp.int32, (BLK, BLK), 1)
            s = jnp.where(qry >= key, s, -jnp.inf)
        p = jnp.exp(s - m) * r
        dp = _dot(v_ref[rows, :], dot_b)
        g = (p * (dp - c) * scale).astype(BF16)
        dk = _dot(g, q_ref[here, :])
        dv = _dot(p.astype(BF16), do_ref[here, :])
        at = pl.ds(j * chips, chips)
        shape = (chips, *dkv_ref.shape[1:3], hd)
        dkv_ref[at, :, :, 0:hd] += dk.reshape(shape)
        dkv_ref[at, :, :, hd : 2 * hd] += dv.reshape(shape)
        return dqt + _dot(kt_ref[j], g)

    dqt = jnp.zeros((hd, BLK), F32)
    dqt = lax.fori_loop(0, i, lambda j, a: step(j, a, False), dqt)
    dqt = step(i, dqt, True)
    dqt_ref[i] = dqt.astype(BF16)
    dq_ref[pl.ds(i * chips, chips)] = jnp.transpose(dqt).astype(BF16).reshape(chips, *dq_ref.shape[1:])


def _torus_messages():
    msgs = {}
    for s in (1, -1):
        msgs["S1", 0, s] = len(msgs)
    for s in (1, -1):
        msgs["F1", 0, s] = len(msgs)
    for a in (0, -1, 1, 2):
        for s in (1, -1):
            msgs["S2", a, s] = len(msgs)
    for a in (0, -1, 1, 2):
        for s in (1, -1):
            msgs["F2", a, s] = len(msgs)
    return msgs


class _TorusGather:
    def __init__(self, n, x_ref, out_ref, l_sem, i_sem, d_sem=None, o_sem=None):
        self.me = me = lax.axis_index("model")
        self.core = lax.rem(me, 2)
        chip = me // 2
        self.side = math.isqrt(n // 2)
        assert self.side == 4
        self.cx, self.cy = lax.rem(chip, self.side), chip // self.side
        self.partner = me + 1 - 2 * self.core
        self.x_ref, self.out_ref, self.i_sem, self.d_sem = x_ref, out_ref, i_sem, d_sem
        self.msgs = _torus_messages()
        self.sent, self.handed, self.handed_in = [], [], []
        self.own = o_sem is not None and pltpu.make_async_remote_copy(
            x_ref, out_ref.at[me], o_sem.at[0], o_sem.at[1], device_id={"model": self.partner}, device_id_type=MESH_ID)
        self.mine = pltpu.make_async_copy(x_ref, out_ref.at[me], l_sem)

    def chip_at(self, dx, dy):
        side = self.side
        return lax.rem(self.cy + dy + side, side) * side + lax.rem(self.cx + dx + side, side)

    def device(self, part, a, b):
        dx, dy = (a, b) if part == 0 else (b, a)
        return self.chip_at(dx, dy) * 2 + self.core

    def region(self, ref, part, hs):
        return ref.at[pl.ds(2 * part + (hs < 0), 2 if hs == 0 else 1)]

    def number(self, m):
        return m[0] * len(self.msgs) + self.msgs[m[1:]]

    def message(self, m):
        part, kind, a, s = m
        i = self.number(m)
        if kind in ("S1", "F1"):
            to = self.device(part, s, 0)
            src = (0, 0) if kind == "S1" else (-s, 0)
        else:
            to = self.device(part, 0, s)
            src = (a, 0) if kind == "S2" else (a, -s)
        hs = s if kind in ("F1", "F2") else 0
        dst = self.out_ref.at[self.device(part, *src)]
        frm = self.x_ref if src == (0, 0) else dst
        return pltpu.make_async_remote_copy(
            self.region(frm, part, hs), self.region(dst, part, hs), self.i_sem.at[0, i], self.i_sem.at[1, i],
            device_id={"model": to}, device_id_type=MESH_ID)

    def piece(self, m, sem):
        part, kind, a, s = m
        i = self.number(m)
        off = {"S1": (-s, 0), "F1": (2, 0), "S2": (a, -s), "F2": (a, 2)}[kind]
        ref = self.region(self.out_ref.at[self.device(part, *off)], part, s if kind in ("F1", "F2") else 0)
        return pltpu.make_async_remote_copy(
            ref, ref, sem.at[0, i], sem.at[1, i], device_id={"model": self.partner}, device_id_type=MESH_ID)

    def send(self, *m):
        self.message(m).start()
        self.sent.append(m)

    def got(self, *m):
        self.piece(m, self.i_sem).wait_recv()
        if self.d_sem is not None:
            self.piece(m, self.d_sem).start()
            self.handed.append(m)

    def start(self):
        for kind in ("S1", "S2"):
            for part in (0, 1):
                for s in (1, -1):
                    self.send(part, kind, 0, s)
        if self.own:
            self.own.start()
        self.mine.start()

    def first(self):
        for s in (1, -1):
            for part in (0, 1):
                self.got(part, "S1", 0, s)
                self.send(part, "F1", 0, s)
                for z in (1, -1):
                    self.send(part, "S2", -s, z)

    def second(self):
        for part in (0, 1):
            for s in (1, -1):
                self.got(part, "F1", 0, s)
            for z in (1, -1):
                self.send(part, "S2", 2, z)

    def third(self, k):
        a, s = (0, -1, 1, 2)[k // 2], (1, -1)[k % 2]
        for part in (0, 1):
            self.got(part, "S2", a, s)
            self.send(part, "F2", a, s)

    def last(self, k):
        a = (0, -1, 1, 2)[k]
        for s in (1, -1):
            for part in (0, 1):
                self.got(part, "F2", a, s)
                if self.d_sem is not None:
                    self.handed_in.append((part, "F2", a, s))
        for m in self.handed_in:
            self.piece(m, self.d_sem).wait_recv()
        self.handed_in = []

    def inner_ready(self):
        self.mine.wait()
        if self.own:
            self.own.wait_recv()
            for part in (0, 1):
                for m in self.msgs:
                    if m[0] != "F2":
                        self.piece((part, *m), self.d_sem).wait_recv()

    def finish(self):
        for m in self.sent:
            self.message(m).wait_send()
        for m in self.handed:
            self.piece(m, self.d_sem).wait_send()
        if self.own:
            self.own.wait_send()


def _step_kernel(n, scale, x_ref, dy_ref, wq_ref, wk_ref, wv_ref, wo_ref,
                 xf_ref, dyf_ref, wqf_ref, dx_ref, dwq_ref, dwk_ref, dwv_ref, dwo_ref,
                 w3_ref, q_ref, k_ref, v_ref, kt_ref, vt_ref, ot_ref, st_ref, do_ref, dq_ref, dqt_ref, s_ref, buf, wbuf,
                 dkv_ref, pbuf, rbuf, all_ref, dqa_ref, xc_ref,
                 xl, xi, xd, xo, yl, yi, yd, yo, wl, wi, b_sem, c_sem, p_sem, q_sem, r_sem, g_sem, f_sem, e_sem, a_sem):
    gx = _TorusGather(n, x_ref, xf_ref, xl, xi, xd, xo)
    gy = _TorusGather(n, dy_ref, dyf_ref, yl, yi, yd, yo)
    gw = _TorusGather(n, wq_ref, wqf_ref, wl, wi)
    me, core, partner = gx.me, gx.core, gx.partner
    chip = me // 2
    nc = n // 2
    d, hd = wk_ref.shape
    nb = st_ref.shape[0]
    per = x_ref.shape[0] * x_ref.shape[1]
    rows = 2 * per

    def dev(idx):
        return {"model": idx}

    def remote(src, dst, sem, to):
        return pltpu.make_async_remote_copy(src, dst, sem[0], sem[1], device_id=dev(to), device_id_type=MESH_ID)

    def peer(o):
        return lax.rem(chip + o, nc) * 2 + core

    barrier = pltpu.get_barrier_semaphore()

    @pl.loop(1, nc)
    def _(o):
        pl.semaphore_signal(barrier, inc=1, device_id=dev(peer(o)), device_id_type=MESH_ID)

    pl.semaphore_signal(barrier, inc=1, device_id=dev(partner), device_id_type=MESH_ID)
    pl.semaphore_wait(barrier, nc)

    gx.start()

    def near(k):
        return gx.chip_at(lax.rem(k, 3) - 1, k // 3 - 1)

    def far(k):
        g = k // 2
        v = jnp.where(g == 3, 2, jnp.where(g == 2, 1, -g))
        even = lax.rem(k, 2) == 0
        return gx.chip_at(jnp.where(even, 2, v), jnp.where(even, v, 2))

    def rows_of(c):
        return pl.ds(pl.multiple_of(c * rows, rows), rows)

    def over_near(src_ref, work):
        def load(k):
            slot = lax.rem(k, 2)
            return pltpu.make_async_copy(src_ref.at[pl.ds(2 * near(k), 2)], buf.at[slot, pl.ds(0, 2)], b_sem.at[slot])

        load(0).start()

        @pl.loop(0, 9)
        def _(k):
            load(k).wait()

            @pl.when(k + 1 < 9)
            def _():
                load(k + 1).start()

            work(buf[lax.rem(k, 2), 0:2].reshape(rows, d), rows_of(near(k)))

    def over_far(g, src_ref, work):
        @pl.loop(0, 7)
        def _(k):
            for z in range(4):
                @pl.when(k == 2 * z)
                def _():
                    g.last(z)

            load = pltpu.make_async_copy(src_ref.at[pl.ds(2 * far(k), 2)], buf.at[0, pl.ds(0, 2)], b_sem.at[0])
            load.start()
            load.wait()
            work(buf[0, 0:2].reshape(rows, d), rows_of(far(k)))

    def project(block, here):
        r = _dot(block, w3_ref[...]).astype(BF16)
        q_ref[here, :] = r[:, :hd]
        k_ref[here, :] = r[:, hd : 2 * hd]
        v_ref[here, :] = r[:, 2 * hd :]

    def project_dy(block, here):
        do_ref[here, :] = lax.dot_general(
            block, wo_ref[...], (((1,), (1,)), ((), ())), preferred_element_type=F32).astype(BF16)

    w3_ref[:, 0:hd] = wq_ref[...].reshape(d, hd)
    w3_ref[:, hd : 2 * hd] = wk_ref[...]
    w3_ref[:, 2 * hd :] = wv_ref[...]
    dkv_ref[...] = jnp.zeros_like(dkv_ref)

    gx.first()
    gx.second()
    for k in range(8):
        gx.third(k)
    gy.start()
    gx.inner_ready()
    over_near(xf_ref, project)
    gy.first()
    over_far(gx, xf_ref, project)
    gy.second()
    cols = pltpu.make_async_copy(
        xf_ref.at[:, :, :, pl.ds(pl.multiple_of(me * (d // n), d // n), d // n)], xc_ref, c_sem)
    cols.start()

    @pl.loop(0, nb)
    def _(j):
        here = pl.ds(pl.multiple_of(j * BLK, BLK), BLK)
        vt_ref[j] = _flip(v_ref[here, :]).astype(BF16)
        kt_ref[j] = _flip(k_ref[here, :]).astype(BF16)

    @pl.loop(0, nb)
    def _(i):
        for k in range(8):
            @pl.when(i == k)
            def _():
                gy.third(k)

        _fwd_block(scale, i, q_ref, k_ref, vt_ref, ot_ref, st_ref, s_ref)

    gw.start()
    gy.inner_ready()
    over_near(dyf_ref, project_dy)
    over_far(gy, dyf_ref, project_dy)

    @pl.loop(0, nb)
    def _(i):
        @pl.when(i == 4)
        def _():
            gw.first()

        @pl.when(i == 6)
        def _():
            gw.second()

        _bwd_block(scale, i, q_ref, do_ref, ot_ref, st_ref, k_ref, v_ref, kt_ref, dq_ref, dqt_ref, dkv_ref)

    pair = remote(dkv_ref.at[:, 1 - core], pbuf, (p_sem.at[0], p_sem.at[1]), partner)
    pair.start()

    def q_copy(o):
        return remote(dq_ref.at[lax.rem(chip + o, nc)], dqa_ref.at[chip], (q_sem.at[0, o], q_sem.at[1, o]), peer(o))

    @pl.loop(1, nc)
    def _(o):
        q_copy(o).start()

    dqa_ref[chip] = dq_ref[chip]
    gw.third(0)
    gw.third(1)
    pair.wait()

    def r_copy(o):
        return remote(pbuf.at[lax.rem(chip + o, nc)], rbuf.at[o], (r_sem.at[0, o], r_sem.at[1, o]), peer(o))

    @pl.loop(1, nc)
    def _(o):
        t = lax.rem(chip + o, nc)
        pbuf[t] += dkv_ref[t, core]
        r_copy(o).start()

    rbuf[0] = pbuf[chip] + dkv_ref[chip, core]

    def over_blocks(src_ref, work, pump):
        def load(j):
            slot = lax.rem(j, 2)
            return pltpu.make_async_copy(src_ref.at[pl.ds(4 * j, 4)], buf.at[slot], b_sem.at[slot])

        load(0).start()

        @pl.loop(0, nb)
        def _(j):
            load(j).wait()

            @pl.when(j + 1 < nb)
            def _():
                load(j + 1).start()

            for at, ks in pump.items():
                @pl.when(j == at)
                def _():
                    for k in ks:
                        gw.third(k)

            @pl.loop(0, nb)
            def _(c):
                work(j, c, buf[lax.rem(j, 2), :, :, :, pl.ds(pl.multiple_of(c * BLK, BLK), BLK)].reshape(BLK, BLK))

    def out_grad(j, c, block):
        here = pl.ds(pl.multiple_of(c * BLK, BLK), BLK)
        r = _dot(ot_ref[j], block)
        dwo_ref[:, here] = jnp.where(j == 0, r, dwo_ref[:, here] + r)

    def query_grad(j, c, block):
        r = _dot(dqt_ref[j], block)
        s_ref[c, 3 * hd : 4 * hd] = jnp.where(j == 0, r, s_ref[c, 3 * hd : 4 * hd] + r)

    dwo_ref[...] = jnp.zeros_like(dwo_ref)
    s_ref[:, 3 * hd : 4 * hd] = jnp.zeros((nb, hd, BLK), F32)
    over_blocks(dyf_ref, out_grad, {0: (2, 3), 4: (4, 5), 7: (6, 7)})

    @pl.loop(1, nc)
    def _(o):
        r_copy(o).wait()
        rbuf[0] += rbuf[o]

    all_ref[me] = rbuf[0].astype(BF16)

    def g_copy(o):
        return remote(all_ref.at[me], all_ref.at[me], (g_sem.at[0, o], g_sem.at[1, o]), peer(o))

    def f_copy(o):
        src = lax.rem(chip + nc - o, nc) * 2 + core
        return remote(all_ref.at[src], all_ref.at[src], (f_sem.at[0, o], f_sem.at[1, o]), partner)

    own = remote(all_ref.at[me], all_ref.at[me], (e_sem.at[0], e_sem.at[1]), partner)

    @pl.loop(1, nc)
    def _(o):
        g_copy(o).start()

    own.start()
    over_blocks(xf_ref, query_grad, {})

    @pl.loop(0, nb)
    def _(c):
        dwq_ref[pl.ds(pl.multiple_of(c * BLK, BLK), BLK), :] = jnp.transpose(s_ref[c, 3 * hd : 4 * hd])

    @pl.loop(1, nc)
    def _(o):
        q_copy(o).wait()

    gw.inner_ready()
    both = (((1,), (1,)), ((), ()))

    def chip_of(k):
        return jnp.where(k < 9, near(k), far(k - 9))

    def add_heads(z):
        c0, c1 = chip_of(2 * z), chip_of(2 * z + 1)
        a = jnp.concatenate([dqa_ref[c0], dqa_ref[c1]], axis=1)

        @pl.loop(0, nb)
        def _(c):
            here = pl.ds(pl.multiple_of(c * BLK, BLK), BLK)
            w = jnp.concatenate([wbuf[0, here, :], wbuf[1, here, :]], axis=1)
            r = lax.dot_general(a, w, both, preferred_element_type=F32)
            s_ref[c, 0:rows] = jnp.where(z == 0, r, s_ref[c, 0:rows] + r)

    s_ref[:, 0:rows] = jnp.zeros((nb, rows, BLK), F32)

    @pl.loop(0, 8)
    def _(z):
        for f in range(4):
            @pl.when(z == 4 + f)
            def _():
                gw.last(f)

        for u in (0, 1):
            pltpu.make_async_copy(
                wqf_ref.at[2 * chip_of(2 * z + u) + core], wbuf.at[u].reshape(wq_ref.shape), b_sem.at[u]).start()
        for u in (0, 1):
            pltpu.make_async_copy(
                wqf_ref.at[2 * chip_of(2 * z + u) + core], wbuf.at[u].reshape(wq_ref.shape), b_sem.at[u]).wait()
        add_heads(z)

    swap = remote(s_ref.at[:, pl.ds(pl.multiple_of((1 - core) * per, per), per)], s_ref.at[:, pl.ds(rows, per)],
                  (a_sem.at[0], a_sem.at[1]), partner)
    swap.start()

    @pl.loop(1, nc)
    def _(o):
        g_copy(o).wait()
        f_copy(o).start()

    own.wait()
    cols.wait()

    @pl.loop(1, nc)
    def _(o):
        f_copy(o).wait()

    def key_grad(j, acc):
        xt = _flip(xc_ref[pl.ds(4 * j, 4)].reshape(BLK, d // n)).astype(BF16)
        return acc + _dot(xt, all_ref[pl.ds(4 * j, 4)].reshape(BLK, 2 * hd))

    r = lax.fori_loop(0, nb, key_grad, jnp.zeros((d // n, 2 * hd), F32))
    dwk_ref[...] = r[:, :hd]
    dwv_ref[...] = r[:, hd:]
    swap.wait()
    mine = all_ref[me]

    @pl.loop(0, nb)
    def _(c):
        here = pl.ds(pl.multiple_of(c * BLK, BLK), BLK)
        w = jnp.concatenate([wk_ref[here, :], wv_ref[here, :]], axis=1)
        r = lax.dot_general(mine, w, both, preferred_element_type=F32)
        at = pl.ds(pl.multiple_of(core * per, per), per)
        dx_ref[:, here] = (s_ref[c, at] + s_ref[c, rows : rows + per] + r).astype(BF16)

    gx.finish()
    gy.finish()
    gw.finish()


def _step(x, dy, wq, wk, wv, wo, n, scale):
    rows, d = x.shape
    hd = wo.shape[0]
    t = n * rows
    nb = t // BLK
    nc = n // 2
    assert nb == 8 and 4 * rows == BLK
    nm = 2 * len(_torus_messages())
    hbm = pl.BlockSpec(memory_space=pltpu.HBM)
    vmem = pl.BlockSpec(memory_space=pltpu.VMEM)
    dma = pltpu.SemaphoreType.DMA
    full = jax.ShapeDtypeStruct((n, 4, rows // 4, d), BF16)
    head = pltpu.VMEM((t, hd), BF16)
    flat = pltpu.VMEM((nb, hd, BLK), BF16)
    return pl.pallas_call(
        functools.partial(_step_kernel, n, scale),
        in_specs=[hbm, hbm] + [vmem] * 4,
        out_specs=[hbm] * 3 + [vmem] * 5,
        out_shape=[
            full, full, jax.ShapeDtypeStruct((n, 4, d // 4, hd), BF16),
            jax.ShapeDtypeStruct((rows, d), BF16), jax.ShapeDtypeStruct((d, hd), F32),
            jax.ShapeDtypeStruct((d // n, hd), F32), jax.ShapeDtypeStruct((d // n, hd), F32),
            jax.ShapeDtypeStruct((hd, d), F32)],
        scratch_shapes=[
            pltpu.VMEM((d, 3 * hd), BF16), head, head, head, flat, flat, flat,
            pltpu.VMEM((nb, 8, BLK), F32), head, pltpu.VMEM((nc, 2 * rows, hd), BF16), flat,
            pltpu.VMEM((nb, BLK, BLK), F32),
            pltpu.VMEM((2, 4, 4, rows // 4, d), BF16),
            pltpu.VMEM((2, d, hd), BF16),
            pltpu.VMEM((nc, 2, rows, 2 * hd), F32),
            pltpu.VMEM((nc, rows, 2 * hd), F32),
            pltpu.VMEM((nc, rows, 2 * hd), F32),
            pltpu.VMEM((n, rows, 2 * hd), BF16),
            pltpu.VMEM((nc, 2 * rows, hd), BF16),
            pltpu.VMEM((n, 4, rows // 4, d // n), BF16),
            dma, dma((2, nm)), dma((2, nm)), dma((2,)),
            dma, dma((2, nm)), dma((2, nm)), dma((2,)),
            dma, dma((2, nm)),
            dma((2,)), dma, dma((2,)), dma((2, nc)), dma((2, nc)), dma((2, nc)), dma((2, nc)), dma((2,)), dma((2,)),
        ],
        compiler_params=pltpu.CompilerParams(collective_id=0, has_side_effects=True, vmem_limit_bytes=67043328),
        cost_estimate=pl.CostEstimate(flops=10**11, bytes_accessed=6 * t * d, transcendentals=t * t),
        name="mqa_backward",
    )(x.reshape(4, rows // 4, d), dy.reshape(4, rows // 4, d), wq.reshape(4, d // 4, hd), wk, wv, wo)


def solution(mesh):
    tok_spec = P(("data", "model"), None)
    n = mesh.shape["model"]

    def local_step(x_loc, dy_loc, wq_loc, w_key, w_value, wo_loc):
        d, hd = w_key.shape
        scale = 1.0 / math.sqrt(hd)
        _, _, _, dx, dwq, dwk, dwv, dwo = _step(
            x_loc, dy_loc, wq_loc.reshape(d, hd), w_key, w_value, wo_loc.reshape(hd, d), n, scale)
        return (dx, dwq[:, None, :], dwk, dwv, dwo[None])

    return jax.shard_map(
        local_step, mesh=mesh,
        in_specs=(tok_spec, tok_spec, P(None, "model", None), P(None, None), P(None, None), P("model", None, None)),
        out_specs=(tok_spec, P("data", "model", None), tok_spec, tok_spec, P(("data", "model"), None, None)),
        check_vma=False)
```

```python
import functools
import math
import jax
import jax.numpy as jnp
from jax import lax
from jax.experimental import pallas as pl
from jax.experimental.pallas import tpu as pltpu
from jax.sharding import PartitionSpec as P

BLK = 512
F32 = jnp.float32
BF16 = jnp.bfloat16
MESH_ID = pl.DeviceIdType.MESH


def _dot(a, b):
    return jnp.dot(a, b, preferred_element_type=F32)


def _flip(a):
    return jnp.transpose(a.astype(F32))


def _fwd_block(scale, i, q_ref, k_ref, vt_ref, ot_ref, st_ref, s_ref):
    here = pl.ds(pl.multiple_of(i * BLK, BLK), BLK)
    qt = _flip(q_ref[here, :]).astype(BF16)

    def score(j, m8, diag):
        s = _dot(k_ref[pl.ds(pl.multiple_of(j * BLK, BLK), BLK), :], qt) * scale
        if diag:
            key = lax.broadcasted_iota(jnp.int32, (BLK, BLK), 0)
            qry = lax.broadcasted_iota(jnp.int32, (BLK, BLK), 1)
            s = jnp.where(qry >= key, s, -jnp.inf)
        s_ref[j] = s
        return jnp.maximum(m8, jnp.max(s.reshape(BLK // 8, 8, BLK), axis=0))

    m8 = jnp.full((8, BLK), -jnp.inf, F32)
    m8 = lax.fori_loop(0, i, lambda j, c: score(j, c, False), m8)
    m8 = score(i, m8, True)
    m = jnp.max(m8, axis=0, keepdims=True)

    def expo(j, l8):
        p = jnp.exp(s_ref[j] - m)
        s_ref[j] = p
        return l8 + jnp.sum(p.reshape(BLK // 8, 8, BLK), axis=0)

    l8 = lax.fori_loop(0, i + 1, expo, jnp.zeros((8, BLK), F32))
    r = 1.0 / jnp.sum(l8, axis=0, keepdims=True)

    def attend(j, ot):
        return ot + _dot(vt_ref[j], (s_ref[j] * r).astype(BF16))

    ot = lax.fori_loop(0, i + 1, attend, jnp.zeros(ot_ref.shape[1:], F32))
    ot_ref[i] = ot.astype(BF16)
    row = lax.broadcasted_iota(jnp.int32, (8, BLK), 0)
    st_ref[i] = jnp.where(row == 0, m, r)


def _bwd_block(scale, i, q_ref, do_ref, ot_ref, st_ref, k_ref, v_ref, kt_ref, dq_ref, dqt_ref, dkv_ref):
    here = pl.ds(pl.multiple_of(i * BLK, BLK), BLK)
    hd = q_ref.shape[1]
    qt = _flip(q_ref[here, :]).astype(BF16)
    dot_f = _flip(do_ref[here, :])
    c = jnp.sum(dot_f * ot_ref[i].astype(F32), axis=0, keepdims=True)
    dot_b = dot_f.astype(BF16)
    m = st_ref[i, 0:1, :]
    r = st_ref[i, 1:2, :]
    chips = BLK // (dkv_ref.shape[1] * dkv_ref.shape[2])

    def step(j, dqt, diag):
        rows = pl.ds(pl.multiple_of(j * BLK, BLK), BLK)
        s = _dot(k_ref[rows, :], qt) * scale
        if diag:
            key = lax.broadcasted_iota(jnp.int32, (BLK, BLK), 0)
            qry = lax.broadcasted_iota(jnp.int32, (BLK, BLK), 1)
            s = jnp.where(qry >= key, s, -jnp.inf)
        p = jnp.exp(s - m) * r
        dp = _dot(v_ref[rows, :], dot_b)
        g = (p * (dp - c) * scale).astype(BF16)
        dk = _dot(g, q_ref[here, :])
        dv = _dot(p.astype(BF16), do_ref[here, :])
        at = pl.ds(j * chips, chips)
        shape = (chips, *dkv_ref.shape[1:3], hd)
        dkv_ref[at, :, :, 0:hd] += dk.reshape(shape)
        dkv_ref[at, :, :, hd : 2 * hd] += dv.reshape(shape)
        return dqt + _dot(kt_ref[j], g)

    dqt = jnp.zeros((hd, BLK), F32)
    dqt = lax.fori_loop(0, i, lambda j, a: step(j, a, False), dqt)
    dqt = step(i, dqt, True)
    dqt_ref[i] = dqt.astype(BF16)
    dq_ref[pl.ds(i * chips, chips)] = jnp.transpose(dqt).astype(BF16).reshape(chips, *dq_ref.shape[1:])


def _torus_messages():
    msgs = {}
    for s in (1, -1):
        msgs["S1", 0, s] = len(msgs)
    for s in (1, -1):
        msgs["F1", 0, s] = len(msgs)
    for a in (0, -1, 1, 2):
        for s in (1, -1):
            msgs["S2", a, s] = len(msgs)
    for a in (0, -1, 1, 2):
        for s in (1, -1):
            msgs["F2", a, s] = len(msgs)
    return msgs


class _TorusGather:
    def __init__(self, n, x_ref, out_ref, l_sem, i_sem, d_sem=None, o_sem=None):
        self.me = me = lax.axis_index("model")
        self.core = lax.rem(me, 2)
        chip = me // 2
        self.side = math.isqrt(n // 2)
        assert self.side == 4
        self.cx, self.cy = lax.rem(chip, self.side), chip // self.side
        self.partner = me + 1 - 2 * self.core
        self.x_ref, self.out_ref, self.i_sem, self.d_sem = x_ref, out_ref, i_sem, d_sem
        self.msgs = _torus_messages()
        self.sent, self.handed, self.handed_in = [], [], []
        self.own = o_sem is not None and pltpu.make_async_remote_copy(
            x_ref, out_ref.at[me], o_sem.at[0], o_sem.at[1], device_id={"model": self.partner}, device_id_type=MESH_ID)
        self.mine = pltpu.make_async_copy(x_ref, out_ref.at[me], l_sem)

    def chip_at(self, dx, dy):
        side = self.side
        return lax.rem(self.cy + dy + side, side) * side + lax.rem(self.cx + dx + side, side)

    def device(self, part, a, b):
        dx, dy = (a, b) if part == 0 else (b, a)
        return self.chip_at(dx, dy) * 2 + self.core

    def region(self, ref, part, hs):
        return ref.at[pl.ds(2 * part + (hs < 0), 2 if hs == 0 else 1)]

    def number(self, m):
        return m[0] * len(self.msgs) + self.msgs[m[1:]]

    def message(self, m):
        part, kind, a, s = m
        i = self.number(m)
        if kind in ("S1", "F1"):
            to = self.device(part, s, 0)
            src = (0, 0) if kind == "S1" else (-s, 0)
        else:
            to = self.device(part, 0, s)
            src = (a, 0) if kind == "S2" else (a, -s)
        hs = s if kind in ("F1", "F2") else 0
        dst = self.out_ref.at[self.device(part, *src)]
        frm = self.x_ref if src == (0, 0) else dst
        return pltpu.make_async_remote_copy(
            self.region(frm, part, hs), self.region(dst, part, hs), self.i_sem.at[0, i], self.i_sem.at[1, i],
            device_id={"model": to}, device_id_type=MESH_ID)

    def piece(self, m, sem):
        part, kind, a, s = m
        i = self.number(m)
        off = {"S1": (-s, 0), "F1": (2, 0), "S2": (a, -s), "F2": (a, 2)}[kind]
        ref = self.region(self.out_ref.at[self.device(part, *off)], part, s if kind in ("F1", "F2") else 0)
        return pltpu.make_async_remote_copy(
            ref, ref, sem.at[0, i], sem.at[1, i], device_id={"model": self.partner}, device_id_type=MESH_ID)

    def send(self, *m):
        self.message(m).start()
        self.sent.append(m)

    def got(self, *m):
        self.piece(m, self.i_sem).wait_recv()
        if self.d_sem is not None:
            self.piece(m, self.d_sem).start()
            self.handed.append(m)

    def start(self):
        for part in (0, 1):
            for s in (1, -1):
                self.send(part, "S1", 0, s)
        if self.own:
            self.own.start()
        self.mine.start()

    def start_cross(self):
        for part in (0, 1):
            for s in (1, -1):
                self.send(part, "S2", 0, s)

    def first(self):
        for s in (1, -1):
            for part in (0, 1):
                self.got(part, "S1", 0, s)
                self.send(part, "F1", 0, s)
                for z in (1, -1):
                    self.send(part, "S2", -s, z)

    def second(self):
        for part in (0, 1):
            for s in (1, -1):
                self.got(part, "F1", 0, s)
            for z in (1, -1):
                self.send(part, "S2", 2, z)

    def third(self, k):
        a, s = (0, -1, 1, 2)[k // 2], (1, -1)[k % 2]
        for part in (0, 1):
            self.got(part, "S2", a, s)
            self.send(part, "F2", a, s)

    def last(self, k):
        a = (0, -1, 1, 2)[k]
        for s in (1, -1):
            for part in (0, 1):
                self.got(part, "F2", a, s)
                if self.d_sem is not None:
                    self.handed_in.append((part, "F2", a, s))
        for m in self.handed_in:
            self.piece(m, self.d_sem).wait_recv()
        self.handed_in = []

    def near_ready(self):
        self.mine.wait()
        if self.own:
            self.own.wait_recv()
            self.ready(lambda m: m[0] == "S1" or (m[0] == "S2" and m[1] != 2))

    def far_ready(self):
        if self.own:
            self.ready(lambda m: m[0] == "F1" or (m[0] == "S2" and m[1] == 2))

    def ready(self, which):
        for part in (0, 1):
            for m in self.msgs:
                if which(m):
                    self.piece((part, *m), self.d_sem).wait_recv()

    def finish(self):
        for m in self.sent:
            self.message(m).wait_send()
        for m in self.handed:
            self.piece(m, self.d_sem).wait_send()
        if self.own:
            self.own.wait_send()


def _step_kernel(n, scale, x_ref, dy_ref, wq_ref, wk_ref, wv_ref, wo_ref,
                 xf_ref, dyf_ref, wqf_ref, dx_ref, dwq_out, dwk_ref, dwv_ref, dwo_out,
                 w3_ref, wov_ref, q_ref, k_ref, v_ref, kt_ref, vt_ref, ot_ref, st_ref, do_ref, dq_ref, dqt_ref, s_ref, buf, wbuf,
                 dkv_ref, pbuf, r1_ref, r2_ref, acc_ref, all_ref, dqa_ref, xc_ref, dwq_ref, dwo_ref,
                 xl, xi, xd, xo, yl, yi, yd, yo, wl, wi, b_sem, w_sem, c_sem, p_sem, q_sem, r1_sem, r2_sem, g1_sem, g2_sem, f_sem, a_sem, o_sem):
    gx = _TorusGather(n, x_ref, xf_ref, xl, xi, xd, xo)
    gy = _TorusGather(n, dy_ref, dyf_ref, yl, yi, yd, yo)
    gw = _TorusGather(n, wq_ref, wqf_ref, wl, wi)
    me, core, partner = gx.me, gx.core, gx.partner
    chip = me // 2
    nc = n // 2
    d, hd = wk_ref.shape
    nb = st_ref.shape[0]
    per = x_ref.shape[0] * x_ref.shape[1]
    rows = 2 * per

    def dev(idx):
        return {"model": idx}

    def remote(src, dst, sem, to):
        return pltpu.make_async_remote_copy(src, dst, sem[0], sem[1], device_id=dev(to), device_id_type=MESH_ID)

    def peer(o):
        return lax.rem(chip + o, nc) * 2 + core

    barrier = pltpu.get_barrier_semaphore()

    @pl.loop(1, nc)
    def _(o):
        pl.semaphore_signal(barrier, inc=1, device_id=dev(peer(o)), device_id_type=MESH_ID)

    pl.semaphore_signal(barrier, inc=1, device_id=dev(partner), device_id_type=MESH_ID)
    pl.semaphore_wait(barrier, nc)

    gx.start()
    weights = [
        pltpu.make_async_copy(wq_ref.reshape(d, hd), w3_ref.at[:, pl.ds(0, hd)], w_sem.at[0]),
        pltpu.make_async_copy(wk_ref, w3_ref.at[:, pl.ds(hd, hd)], w_sem.at[1]),
        pltpu.make_async_copy(wv_ref, w3_ref.at[:, pl.ds(2 * hd, hd)], w_sem.at[2]),
        pltpu.make_async_copy(wo_ref, wov_ref, w_sem.at[3]),
    ]
    for w in weights:
        w.start()
    gx.start_cross()

    def near(k):
        return gx.chip_at(lax.rem(k, 3) - 1, k // 3 - 1)

    def far(k):
        g = k // 2
        v = jnp.where(g == 3, 2, jnp.where(g == 2, 1, -g))
        even = lax.rem(k, 2) == 0
        return gx.chip_at(jnp.where(even, 2, v), jnp.where(even, v, 2))

    def rows_of(c):
        return pl.ds(pl.multiple_of(c * rows, rows), rows)

    def load_chip(src_ref, c, slot):
        return [pltpu.make_async_copy(src_ref.at[2 * c + u], buf.at[slot, u], b_sem.at[slot, u]) for u in (0, 1)]

    def over_near(src_ref, work):
        def load(k):
            return load_chip(src_ref, near(k), lax.rem(k, 2))

        for cp in load(0):
            cp.start()

        @pl.loop(0, 9)
        def _(k):
            for cp in load(k):
                cp.wait()

            @pl.when(k + 1 < 9)
            def _():
                for cp in load(k + 1):
                    cp.start()

            work(lax.rem(k, 2), near(k))

    def over_far(g, src_ref, work, hook=None):
        def load(k):
            return load_chip(src_ref, far(k), lax.rem(k, 2))

        @pl.loop(0, 7)
        def _(k):
            for z in range(4):
                @pl.when(k == 2 * z)
                def _():
                    if z == 3 and hook is not None:
                        hook()
                    g.last(z)
                    for cp in load(k):
                        cp.start()
                    if z < 3:
                        for cp in load(k + 1):
                            cp.start()

            for cp in load(k):
                cp.wait()
            work(lax.rem(k, 2), far(k))

    def project(slot, c):
        here = rows_of(c)
        r = _dot(buf[slot, 0:2].reshape(rows, d), w3_ref[...]).astype(BF16)
        q_ref[here, :] = r[:, :hd]
        k_ref[here, :] = r[:, hd : 2 * hd]
        v_ref[here, :] = r[:, 2 * hd :]

    def project_dy(slot, c):
        do_ref[rows_of(c), :] = lax.dot_general(
            buf[slot, 0:2].reshape(rows, d), wov_ref[...], (((1,), (1,)), ((), ())),
            preferred_element_type=F32).astype(BF16)

    dkv_ref[...] = jnp.zeros_like(dkv_ref)
    dwo_ref[...] = jnp.zeros_like(dwo_ref)

    gx.first()
    for w in weights:
        w.wait()
    gx.second()
    for k in range(8):
        gx.third(k)
    gy.start()
    gx.near_ready()
    over_near(xf_ref, project)
    gy.start_cross()
    gx.far_ready()
    over_far(gx, xf_ref, project)
    gy.first()
    own_cols = pltpu.make_async_copy(
        xf_ref.at[:, :, :, pl.ds(pl.multiple_of(me * (d // n), d // n), d // n)], xc_ref, c_sem)
    own_cols.start()

    @pl.loop(0, nb)
    def _(j):
        here = pl.ds(pl.multiple_of(j * BLK, BLK), BLK)
        vt_ref[j] = _flip(v_ref[here, :]).astype(BF16)
        kt_ref[j] = _flip(k_ref[here, :]).astype(BF16)

    @pl.loop(0, nb)
    def _(i):
        @pl.when(i == 5)
        def _():
            gy.third(0)
            gy.third(1)

        _fwd_block(scale, i, q_ref, k_ref, vt_ref, ot_ref, st_ref, s_ref)

    gy.second()
    for k in range(2, 6):
        gy.third(k)
    gw.start()
    gy.near_ready()
    over_near(dyf_ref, project_dy)
    gy.third(6)
    gy.third(7)
    gw.start_cross()
    gy.far_ready()
    over_far(gy, dyf_ref, project_dy, gw.first)

    @pl.loop(0, nb)
    def _(i):
        @pl.when(i == 5)
        def _():
            gw.third(0)
            gw.third(1)

        _bwd_block(scale, i, q_ref, do_ref, ot_ref, st_ref, k_ref, v_ref, kt_ref, dq_ref, dqt_ref, dkv_ref)

    pair = remote(dkv_ref.at[:, 1 - core], pbuf, (p_sem.at[0], p_sem.at[1]), partner)
    pair.start()
    dqa_ref[chip] = dq_ref[chip]
    pair.wait()
    side = gx.side
    here = (gx.cx, gx.cy)
    lanes = (pl.ds(0, hd), pl.ds(hd, hd))
    psum = pbuf.reshape(side, side, per, 2 * hd)

    @pl.loop(0, nc)
    def _(t):
        pbuf[t] += dkv_ref[t, core]

    def sems(ref, part, o):
        return ref.at[0, part, o], ref.at[1, part, o]

    def r1_copy(part, o):
        to = lax.rem(here[part] + o, side)
        src = psum.at[:, to, :, lanes[part]] if part == 0 else psum.at[to, :, :, lanes[part]]
        return remote(src, r1_ref.at[part, o], sems(r1_sem, part, o), gx.device(part, o, 0))

    def r2_copy(part, o):
        to = lax.rem(here[1 - part] + o, side)
        return remote(acc_ref.at[part, to], r2_ref.at[part, o], sems(r2_sem, part, o), gx.device(part, 0, o))

    def g1_copy(part, o):
        ref = all_ref.at[me, :, lanes[part]]
        return remote(ref, ref, sems(g1_sem, part, o), gx.device(part, o, 0))

    def g2_copy(part, o):
        whole = all_ref.reshape(side, side, 2, per, 2 * hd)
        ref = whole.at[gx.cy, :, core, :, lanes[0]] if part == 0 else whole.at[:, gx.cx, core, :, lanes[1]]
        return remote(ref, ref, sems(g2_sem, part, o), gx.device(part, 0, o))

    def each(make, act):
        for part in (0, 1):
            for o in range(1, side):
                getattr(make(part, o), act)()

    def q_copy(o):
        return remote(dq_ref.at[lax.rem(chip + o, nc)], dqa_ref.at[chip], (q_sem.at[0, o], q_sem.at[1, o]), peer(o))

    each(r1_copy, "start")
    gw.second()

    def over_blocks(src_ref, work, pump):
        def load(j):
            slot = lax.rem(j, 2)
            return [pltpu.make_async_copy(
                src_ref.at[pl.ds(4 * j + 2 * u, 2)], buf.at[slot, pl.ds(2 * u, 2)], b_sem.at[slot, u]) for u in (0, 1)]

        for cp in load(0):
            cp.start()

        @pl.loop(0, nb)
        def _(j):
            for cp in load(j):
                cp.wait()

            @pl.when(j + 1 < nb)
            def _():
                for cp in load(j + 1):
                    cp.start()

            for at, ks in pump.items():
                @pl.when(j == at)
                def _():
                    for k in ks:
                        gw.third(k)

            @pl.loop(0, nb)
            def _(c):
                cols = pl.ds(pl.multiple_of(c * BLK, BLK), BLK)
                work(j, c, cols, buf[lax.rem(j, 2), :, :, :, cols].reshape(BLK, BLK))

    def out_grad(j, c, at, block):
        dwo_ref[:, at] += _dot(ot_ref[j], block)

    def query_grad(j, c, at, block):
        s_ref[c, 3 * hd : 4 * hd] += _dot(dqt_ref[j], block)

    s_ref[:, 3 * hd : 4 * hd] = jnp.zeros((nb, hd, BLK), F32)
    s_ref[:, 0:rows] = jnp.zeros((nb, rows, BLK), F32)
    over_blocks(dyf_ref, out_grad, {0: (2, 3), 3: (4, 5)})
    out_store = pltpu.make_async_copy(dwo_ref, dwo_out, o_sem.at[0])
    out_store.start()
    each(r1_copy, "wait")
    for z in range(side):
        for part in (0, 1):
            got = psum[z, gx.cx, :, 0:hd] if part == 0 else psum[gx.cy, z, :, hd:]
            for o in range(1, side):
                got = got + r1_ref[part, o, z]
            acc_ref[part, z] = got
    each(r2_copy, "start")

    @pl.loop(1, nc)
    def _(o):
        q_copy(o).start()

    over_blocks(xf_ref, query_grad, {2: (6, 7)})
    each(r2_copy, "wait")
    for part in (0, 1):
        got = acc_ref[part, here[1 - part]]
        for o in range(1, side):
            got = got + r2_ref[part, o]
        all_ref[me, :, part * hd : (part + 1) * hd] = got.astype(BF16)
    each(g1_copy, "start")

    @pl.loop(0, nb)
    def _(c):
        dwq_ref[pl.ds(pl.multiple_of(c * BLK, BLK), BLK), :] = jnp.transpose(s_ref[c, 3 * hd : 4 * hd])

    query_store = pltpu.make_async_copy(dwq_ref, dwq_out, o_sem.at[1])
    query_store.start()
    each(g1_copy, "wait")
    each(g2_copy, "start")

    @pl.loop(1, nc)
    def _(o):
        q_copy(o).wait()

    both = (((1,), (1,)), ((), ()))

    def chip_of(k):
        return jnp.where(k < 9, near(k), far(k - 9))

    def add_heads(z):
        a = jnp.concatenate([dqa_ref[chip_of(2 * z)], dqa_ref[chip_of(2 * z + 1)]], axis=1)

        @pl.loop(0, nb)
        def _(c):
            here = pl.ds(pl.multiple_of(c * BLK, BLK), BLK)
            slot = lax.rem(z, 2)
            w = jnp.concatenate([wbuf[slot, 0, here, :], wbuf[slot, 1, here, :]], axis=1)
            s_ref[c, 0:rows] += lax.dot_general(a, w, both, preferred_element_type=F32)

    def load_heads(z):
        return [pltpu.make_async_copy(
            wqf_ref.at[2 * chip_of(2 * z + u) + core], wbuf.at[lax.rem(z, 2), u].reshape(wq_ref.shape),
            b_sem.at[lax.rem(z, 2), u]) for u in (0, 1)]

    gw.near_ready()
    for cp in load_heads(0):
        cp.start()

    @pl.loop(0, 4)
    def _(z):
        for cp in load_heads(z):
            cp.wait()

        @pl.when(z + 1 < 4)
        def _():
            for cp in load_heads(z + 1):
                cp.start()

        add_heads(z)

    each(g2_copy, "wait")
    hand_all = remote(all_ref.reshape(nc, 2, per, 2 * hd).at[:, core], all_ref.reshape(nc, 2, per, 2 * hd).at[:, core],
                      (f_sem.at[0], f_sem.at[1]), partner)
    hand_all.start()

    @pl.loop(4, 8)
    def _(z):
        for f in range(4):
            @pl.when(z == 4 + f)
            def _():
                gw.last(f)

        for cp in load_heads(z):
            cp.start()
        for cp in load_heads(z):
            cp.wait()
        add_heads(z)

    swap = remote(s_ref.at[:, pl.ds(pl.multiple_of((1 - core) * per, per), per)], s_ref.at[:, pl.ds(rows, per)],
                  (a_sem.at[0], a_sem.at[1]), partner)
    swap.start()
    hand_all.wait()
    own_cols.wait()

    def key_grad(j, acc):
        xt = _flip(xc_ref[pl.ds(4 * j, 4)].reshape(BLK, d // n)).astype(BF16)
        return acc + _dot(xt, all_ref[pl.ds(4 * j, 4)].reshape(BLK, 2 * hd))

    r = lax.fori_loop(0, nb, key_grad, jnp.zeros((d // n, 2 * hd), F32))
    dwk_ref[...] = r[:, :hd]
    dwv_ref[...] = r[:, hd:]
    swap.wait()
    mine = all_ref[me]

    @pl.loop(0, nb)
    def _(c):
        here = pl.ds(pl.multiple_of(c * BLK, BLK), BLK)
        r = lax.dot_general(mine, w3_ref[here, hd:], both, preferred_element_type=F32)
        at = pl.ds(pl.multiple_of(core * per, per), per)
        dx_ref[:, here] = (s_ref[c, at] + s_ref[c, rows : rows + per] + r).astype(BF16)

    gx.finish()
    gy.finish()
    gw.finish()
    out_store.wait()
    query_store.wait()


def _step(x, dy, wq, wk, wv, wo, n, scale):
    rows, d = x.shape
    hd = wo.shape[0]
    t = n * rows
    nb = t // BLK
    nc = n // 2
    assert nb == 8 and 4 * rows == BLK
    nm = 2 * len(_torus_messages())
    hbm = pl.BlockSpec(memory_space=pltpu.HBM)
    vmem = pl.BlockSpec(memory_space=pltpu.VMEM)
    dma = pltpu.SemaphoreType.DMA
    full = jax.ShapeDtypeStruct((n, 4, rows // 4, d), BF16)
    head = pltpu.VMEM((t, hd), BF16)
    flat = pltpu.VMEM((nb, hd, BLK), BF16)
    return pl.pallas_call(
        functools.partial(_step_kernel, n, scale),
        in_specs=[hbm] * 6,
        out_specs=[hbm] * 3 + [vmem, hbm, vmem, vmem, hbm],
        out_shape=[
            full, full, jax.ShapeDtypeStruct((n, 4, d // 4, hd), BF16),
            jax.ShapeDtypeStruct((rows, d), BF16), jax.ShapeDtypeStruct((d, hd), F32),
            jax.ShapeDtypeStruct((d // n, hd), F32), jax.ShapeDtypeStruct((d // n, hd), F32),
            jax.ShapeDtypeStruct((hd, d), F32)],
        scratch_shapes=[
            pltpu.VMEM((d, 3 * hd), BF16), pltpu.VMEM((hd, d), BF16), head, head, head, flat, flat, flat,
            pltpu.VMEM((nb, 8, BLK), F32), head, pltpu.VMEM((nc, 2 * rows, hd), BF16), flat,
            pltpu.VMEM((nb, BLK, BLK), F32),
            pltpu.VMEM((2, 4, 4, rows // 4, d), BF16),
            pltpu.VMEM((2, 2, d, hd), BF16),
            pltpu.VMEM((nc, 2, rows, 2 * hd), F32),
            pltpu.VMEM((nc, rows, 2 * hd), F32),
            pltpu.VMEM((2, 4, 4, rows, hd), F32), pltpu.VMEM((2, 4, rows, hd), F32), pltpu.VMEM((2, 4, rows, hd), F32),
            pltpu.VMEM((n, rows, 2 * hd), BF16),
            pltpu.VMEM((nc, 2 * rows, hd), BF16),
            pltpu.VMEM((n, 4, rows // 4, d // n), BF16),
            pltpu.VMEM((d, hd), F32), pltpu.VMEM((hd, d), F32),
            dma, dma((2, nm)), dma((2, nm)), dma((2,)),
            dma, dma((2, nm)), dma((2, nm)), dma((2,)),
            dma, dma((2, nm)),
            dma((2, 2)), dma((4,)), dma, dma((2,)), dma((2, nc)), *[dma((2, 2, 4))] * 4, dma((2,)), dma((2,)), dma((2,)),
        ],
        compiler_params=pltpu.CompilerParams(collective_id=0, has_side_effects=True, vmem_limit_bytes=67043328),
        cost_estimate=pl.CostEstimate(flops=10**11, bytes_accessed=6 * t * d, transcendentals=t * t),
        name="mqa_backward",
    )(x.reshape(4, rows // 4, d), dy.reshape(4, rows // 4, d), wq.reshape(4, d // 4, hd), wk, wv, wo)


def solution(mesh):
    tok_spec = P(("data", "model"), None)
    n = mesh.shape["model"]

    def local_step(x_loc, dy_loc, wq_loc, w_key, w_value, wo_loc):
        d, hd = w_key.shape
        scale = 1.0 / math.sqrt(hd)
        _, _, _, dx, dwq, dwk, dwv, dwo = _step(
            x_loc, dy_loc, wq_loc.reshape(d, hd), w_key, w_value, wo_loc.reshape(hd, d), n, scale)
        return (dx, dwq[:, None, :], dwk, dwv, dwo[None])

    return jax.shard_map(
        local_step, mesh=mesh,
        in_specs=(tok_spec, tok_spec, P(None, "model", None), P(None, None), P(None, None), P("model", None, None)),
        out_specs=(tok_spec, P("data", "model", None), tok_spec, tok_spec, P(("data", "model"), None, None)),
        check_vma=False)
```

```python
import functools
import math
import jax
import jax.numpy as jnp
from jax import lax
from jax.experimental import pallas as pl
from jax.experimental.pallas import tpu as pltpu
from jax.sharding import PartitionSpec as P

BLK = 512
F32 = jnp.float32
BF16 = jnp.bfloat16
MESH_ID = pl.DeviceIdType.MESH


def _dot(a, b):
    return jnp.dot(a, b, preferred_element_type=F32)


def _flip(a):
    return jnp.transpose(a.astype(F32))


def _fwd_block(scale, i, q_ref, k_ref, vt_ref, ot_ref, st_ref, s_ref):
    here = pl.ds(pl.multiple_of(i * BLK, BLK), BLK)
    qt = _flip(q_ref[here, :]).astype(BF16)

    def score(j, m8, diag):
        s = _dot(k_ref[pl.ds(pl.multiple_of(j * BLK, BLK), BLK), :], qt) * scale
        if diag:
            key = lax.broadcasted_iota(jnp.int32, (BLK, BLK), 0)
            qry = lax.broadcasted_iota(jnp.int32, (BLK, BLK), 1)
            s = jnp.where(qry >= key, s, -jnp.inf)
        s_ref[j] = s
        return jnp.maximum(m8, jnp.max(s.reshape(BLK // 8, 8, BLK), axis=0))

    m8 = jnp.full((8, BLK), -jnp.inf, F32)
    m8 = lax.fori_loop(0, i, lambda j, c: score(j, c, False), m8)
    m8 = score(i, m8, True)
    m = jnp.max(m8, axis=0, keepdims=True)

    def expo(j, l8):
        p = jnp.exp(s_ref[j] - m)
        s_ref[j] = p
        return l8 + jnp.sum(p.reshape(BLK // 8, 8, BLK), axis=0)

    l8 = lax.fori_loop(0, i + 1, expo, jnp.zeros((8, BLK), F32))
    r = 1.0 / jnp.sum(l8, axis=0, keepdims=True)

    def attend(j, ot):
        return ot + _dot(vt_ref[j], (s_ref[j] * r).astype(BF16))

    ot = lax.fori_loop(0, i + 1, attend, jnp.zeros(ot_ref.shape[1:], F32))
    ot_ref[i] = ot.astype(BF16)
    row = lax.broadcasted_iota(jnp.int32, (8, BLK), 0)
    st_ref[i] = jnp.where(row == 0, m, r)


def _bwd_block(scale, i, q_ref, do_ref, ot_ref, st_ref, k_ref, v_ref, kt_ref, dq_ref, dqt_ref, dkv_ref):
    here = pl.ds(pl.multiple_of(i * BLK, BLK), BLK)
    hd = q_ref.shape[1]
    qt = _flip(q_ref[here, :]).astype(BF16)
    dot_f = _flip(do_ref[here, :])
    c = jnp.sum(dot_f * ot_ref[i].astype(F32), axis=0, keepdims=True)
    dot_b = dot_f.astype(BF16)
    m = st_ref[i, 0:1, :]
    r = st_ref[i, 1:2, :]
    chips = BLK // (dkv_ref.shape[1] * dkv_ref.shape[2])

    def step(j, dqt, diag):
        rows = pl.ds(pl.multiple_of(j * BLK, BLK), BLK)
        s = _dot(k_ref[rows, :], qt) * scale
        if diag:
            key = lax.broadcasted_iota(jnp.int32, (BLK, BLK), 0)
            qry = lax.broadcasted_iota(jnp.int32, (BLK, BLK), 1)
            s = jnp.where(qry >= key, s, -jnp.inf)
        p = jnp.exp(s - m) * r
        dp = _dot(v_ref[rows, :], dot_b)
        g = (p * (dp - c) * scale).astype(BF16)
        dk = _dot(g, q_ref[here, :])
        dv = _dot(p.astype(BF16), do_ref[here, :])
        at = pl.ds(j * chips, chips)
        shape = (chips, *dkv_ref.shape[1:3], hd)
        dkv_ref[at, :, :, 0:hd] += dk.reshape(shape)
        dkv_ref[at, :, :, hd : 2 * hd] += dv.reshape(shape)
        return dqt + _dot(kt_ref[j], g)

    dqt = jnp.zeros((hd, BLK), F32)
    dqt = lax.fori_loop(0, i, lambda j, a: step(j, a, False), dqt)
    dqt = step(i, dqt, True)
    dqt_ref[i] = dqt.astype(BF16)
    dq_ref[pl.ds(i * chips, chips)] = jnp.transpose(dqt).astype(BF16).reshape(chips, *dq_ref.shape[1:])


def _torus_messages():
    msgs = {}
    for s in (1, -1):
        msgs["S1", 0, s] = len(msgs)
    for s in (1, -1):
        msgs["F1", 0, s] = len(msgs)
    for a in (0, -1, 1, 2):
        for s in (1, -1):
            msgs["S2", a, s] = len(msgs)
    for a in (0, -1, 1, 2):
        for s in (1, -1):
            msgs["F2", a, s] = len(msgs)
    return msgs


class _TorusGather:
    def __init__(self, n, x_ref, out_ref, l_sem, i_sem, d_sem=None, o_sem=None):
        self.me = me = lax.axis_index("model")
        self.core = lax.rem(me, 2)
        chip = me // 2
        self.side = math.isqrt(n // 2)
        assert self.side == 4
        self.cx, self.cy = lax.rem(chip, self.side), chip // self.side
        self.partner = me + 1 - 2 * self.core
        self.x_ref, self.out_ref, self.i_sem, self.d_sem = x_ref, out_ref, i_sem, d_sem
        self.msgs = _torus_messages()
        self.sent, self.handed, self.handed_in = [], [], []
        self.own = o_sem is not None and pltpu.make_async_remote_copy(
            x_ref, out_ref.at[me], o_sem.at[0], o_sem.at[1], device_id={"model": self.partner}, device_id_type=MESH_ID)
        self.mine = pltpu.make_async_copy(x_ref, out_ref.at[me], l_sem)

    def chip_at(self, dx, dy):
        side = self.side
        return lax.rem(self.cy + dy + side, side) * side + lax.rem(self.cx + dx + side, side)

    def device(self, part, a, b):
        dx, dy = (a, b) if part == 0 else (b, a)
        return self.chip_at(dx, dy) * 2 + self.core

    def region(self, ref, part, hs):
        return ref.at[pl.ds(2 * part + (hs < 0), 2 if hs == 0 else 1)]

    def number(self, m):
        return m[0] * len(self.msgs) + self.msgs[m[1:]]

    def message(self, m):
        part, kind, a, s = m
        i = self.number(m)
        if kind in ("S1", "F1"):
            to = self.device(part, s, 0)
            src = (0, 0) if kind == "S1" else (-s, 0)
        else:
            to = self.device(part, 0, s)
            src = (a, 0) if kind == "S2" else (a, -s)
        hs = s if kind in ("F1", "F2") else 0
        dst = self.out_ref.at[self.device(part, *src)]
        frm = self.x_ref if src == (0, 0) else dst
        return pltpu.make_async_remote_copy(
            self.region(frm, part, hs), self.region(dst, part, hs), self.i_sem.at[0, i], self.i_sem.at[1, i],
            device_id={"model": to}, device_id_type=MESH_ID)

    def piece(self, m, sem):
        part, kind, a, s = m
        i = self.number(m)
        off = {"S1": (-s, 0), "F1": (2, 0), "S2": (a, -s), "F2": (a, 2)}[kind]
        ref = self.region(self.out_ref.at[self.device(part, *off)], part, s if kind in ("F1", "F2") else 0)
        return pltpu.make_async_remote_copy(
            ref, ref, sem.at[0, i], sem.at[1, i], device_id={"model": self.partner}, device_id_type=MESH_ID)

    def send(self, *m):
        self.message(m).start()
        self.sent.append(m)

    def got(self, *m):
        self.piece(m, self.i_sem).wait_recv()
        if self.d_sem is not None:
            self.piece(m, self.d_sem).start()
            self.handed.append(m)

    def start(self):
        for part in (0, 1):
            for s in (1, -1):
                self.send(part, "S1", 0, s)
        if self.own:
            self.own.start()
        self.mine.start()

    def start_cross(self):
        for part in (0, 1):
            for s in (1, -1):
                self.send(part, "S2", 0, s)

    def first(self):
        for s in (1, -1):
            for part in (0, 1):
                self.got(part, "S1", 0, s)
                self.send(part, "F1", 0, s)
                for z in (1, -1):
                    self.send(part, "S2", -s, z)

    def second(self):
        for part in (0, 1):
            for s in (1, -1):
                self.got(part, "F1", 0, s)
            for z in (1, -1):
                self.send(part, "S2", 2, z)

    def third(self, k):
        a, s = (0, -1, 1, 2)[k // 2], (1, -1)[k % 2]
        for part in (0, 1):
            self.got(part, "S2", a, s)
            self.send(part, "F2", a, s)

    def last(self, k):
        a = (0, -1, 1, 2)[k]
        for s in (1, -1):
            for part in (0, 1):
                self.got(part, "F2", a, s)
                if self.d_sem is not None:
                    self.handed_in.append((part, "F2", a, s))
        for m in self.handed_in:
            self.piece(m, self.d_sem).wait_recv()
        self.handed_in = []

    def near_ready(self):
        self.mine.wait()
        if self.own:
            self.own.wait_recv()
            self.ready(lambda m: m[0] == "S1" or (m[0] == "S2" and m[1] != 2))

    def far_ready(self):
        if self.own:
            self.ready(lambda m: m[0] == "F1" or (m[0] == "S2" and m[1] == 2))

    def ready(self, which):
        for part in (0, 1):
            for m in self.msgs:
                if which(m):
                    self.piece((part, *m), self.d_sem).wait_recv()

    def finish(self):
        for m in self.sent:
            self.message(m).wait_send()
        for m in self.handed:
            self.piece(m, self.d_sem).wait_send()
        if self.own:
            self.own.wait_send()


def _step_kernel(n, scale, x_ref, dy_ref, wq_ref, wk_ref, wv_ref, wo_ref,
                 xf_ref, dyf_ref, wqf_ref, dx_ref, dwq_out, dwk_ref, dwv_ref, dwo_out,
                 w3_ref, wov_ref, q_ref, k_ref, v_ref, kt_ref, vt_ref, ot_ref, st_ref, do_ref, dq_ref, dqt_ref, s_ref, buf, wbuf,
                 dkv_ref, pbuf, r1_ref, r2_ref, acc_ref, all_ref, dqa_ref, xc_ref, dwq_ref, dwo_ref,
                 xl, xi, xd, xo, yl, yi, yd, yo, wl, wi, b_sem, w_sem, c_sem, p_sem, q_sem, r1_sem, r2_sem, g1_sem, g2_sem, f_sem, a_sem, o_sem):
    gx = _TorusGather(n, x_ref, xf_ref, xl, xi, xd, xo)
    gy = _TorusGather(n, dy_ref, dyf_ref, yl, yi, yd, yo)
    gw = _TorusGather(n, wq_ref, wqf_ref, wl, wi)
    me, core, partner = gx.me, gx.core, gx.partner
    chip = me // 2
    nc = n // 2
    d, hd = wk_ref.shape
    nb = st_ref.shape[0]
    per = x_ref.shape[0] * x_ref.shape[1]
    rows = 2 * per

    def dev(idx):
        return {"model": idx}

    def remote(src, dst, sem, to):
        return pltpu.make_async_remote_copy(src, dst, sem[0], sem[1], device_id=dev(to), device_id_type=MESH_ID)

    def peer(o):
        return lax.rem(chip + o, nc) * 2 + core

    barrier = pltpu.get_barrier_semaphore()

    @pl.loop(1, nc)
    def _(o):
        pl.semaphore_signal(barrier, inc=1, device_id=dev(peer(o)), device_id_type=MESH_ID)

    pl.semaphore_signal(barrier, inc=1, device_id=dev(partner), device_id_type=MESH_ID)
    pl.semaphore_wait(barrier, nc)

    gx.start()
    weights = [
        pltpu.make_async_copy(wq_ref.reshape(d, hd), w3_ref.at[:, pl.ds(0, hd)], w_sem.at[0]),
        pltpu.make_async_copy(wk_ref, w3_ref.at[:, pl.ds(hd, hd)], w_sem.at[1]),
        pltpu.make_async_copy(wv_ref, w3_ref.at[:, pl.ds(2 * hd, hd)], w_sem.at[2]),
        pltpu.make_async_copy(wo_ref, wov_ref, w_sem.at[3]),
    ]
    for w in weights:
        w.start()
    gx.start_cross()

    def near(k):
        return gx.chip_at(lax.rem(k, 3) - 1, k // 3 - 1)

    def far(k):
        g = k // 2
        v = jnp.where(g == 3, 2, jnp.where(g == 2, 1, -g))
        even = lax.rem(k, 2) == 0
        return gx.chip_at(jnp.where(even, 2, v), jnp.where(even, v, 2))

    def rows_of(c):
        return pl.ds(pl.multiple_of(c * rows, rows), rows)

    def load_chip(src_ref, c, slot):
        return [pltpu.make_async_copy(src_ref.at[2 * c + u], buf.at[slot, u], b_sem.at[slot, u]) for u in (0, 1)]

    def over_near(src_ref, work):
        def load(k):
            return load_chip(src_ref, near(k), lax.rem(k, 2))

        for cp in load(0):
            cp.start()

        @pl.loop(0, 9)
        def _(k):
            for cp in load(k):
                cp.wait()

            @pl.when(k + 1 < 9)
            def _():
                for cp in load(k + 1):
                    cp.start()

            work(lax.rem(k, 2), near(k))

    def over_far(g, src_ref, work, hook=None):
        def load(k):
            return load_chip(src_ref, far(k), lax.rem(k, 2))

        @pl.loop(0, 7)
        def _(k):
            for z in range(4):
                @pl.when(k == 2 * z)
                def _():
                    if z == 3 and hook is not None:
                        hook()
                    g.last(z)
                    for cp in load(k):
                        cp.start()
                    if z < 3:
                        for cp in load(k + 1):
                            cp.start()

            for cp in load(k):
                cp.wait()
            work(lax.rem(k, 2), far(k))

    def project(slot, c):
        here = rows_of(c)
        r = _dot(buf[slot, 0:2].reshape(rows, d), w3_ref[...]).astype(BF16)
        q_ref[here, :] = r[:, :hd]
        k_ref[here, :] = r[:, hd : 2 * hd]
        v_ref[here, :] = r[:, 2 * hd :]

    def project_dy(slot, c):
        do_ref[rows_of(c), :] = lax.dot_general(
            buf[slot, 0:2].reshape(rows, d), wov_ref[...], (((1,), (1,)), ((), ())),
            preferred_element_type=F32).astype(BF16)

    dkv_ref[...] = jnp.zeros_like(dkv_ref)
    dwo_ref[...] = jnp.zeros_like(dwo_ref)

    gx.first()
    for w in weights:
        w.wait()
    gx.second()
    for k in range(8):
        gx.third(k)
    gy.start()
    gx.near_ready()
    over_near(xf_ref, project)
    gy.start_cross()
    gx.far_ready()
    over_far(gx, xf_ref, project)
    gy.first()
    own_cols = pltpu.make_async_copy(
        xf_ref.at[:, :, :, pl.ds(pl.multiple_of(me * (d // n), d // n), d // n)], xc_ref, c_sem)
    own_cols.start()

    @pl.loop(0, nb)
    def _(j):
        here = pl.ds(pl.multiple_of(j * BLK, BLK), BLK)
        vt_ref[j] = _flip(v_ref[here, :]).astype(BF16)
        kt_ref[j] = _flip(k_ref[here, :]).astype(BF16)

    @pl.loop(0, nb)
    def _(i):
        @pl.when(i == 5)
        def _():
            gy.third(0)
            gy.third(1)

        _fwd_block(scale, i, q_ref, k_ref, vt_ref, ot_ref, st_ref, s_ref)

    gy.second()
    for k in range(2, 6):
        gy.third(k)
    gw.start()
    gy.near_ready()
    over_near(dyf_ref, project_dy)
    gy.third(6)
    gy.third(7)
    gw.start_cross()
    gy.far_ready()
    over_far(gy, dyf_ref, project_dy, gw.first)

    @pl.loop(0, nb)
    def _(i):
        @pl.when(i == 5)
        def _():
            gw.third(0)
            gw.third(1)

        _bwd_block(scale, i, q_ref, do_ref, ot_ref, st_ref, k_ref, v_ref, kt_ref, dq_ref, dqt_ref, dkv_ref)

    pair = remote(dkv_ref.at[:, 1 - core], pbuf, (p_sem.at[0], p_sem.at[1]), partner)
    pair.start()
    dqa_ref[chip] = dq_ref[chip]
    pair.wait()
    side = gx.side
    here = (gx.cx, gx.cy)
    lanes = (pl.ds(0, hd), pl.ds(hd, hd))
    psum = pbuf.reshape(side, side, per, 2 * hd)

    @pl.loop(0, nc)
    def _(t):
        pbuf[t] += dkv_ref[t, core]

    def sems(ref, part, o):
        return ref.at[0, part, o], ref.at[1, part, o]

    def r1_copy(part, o):
        to = lax.rem(here[part] + o, side)
        src = psum.at[:, to, :, lanes[part]] if part == 0 else psum.at[to, :, :, lanes[part]]
        return remote(src, r1_ref.at[part, o], sems(r1_sem, part, o), gx.device(part, o, 0))

    def r2_copy(part, o):
        to = lax.rem(here[1 - part] + o, side)
        return remote(acc_ref.at[part, to], r2_ref.at[part, o], sems(r2_sem, part, o), gx.device(part, 0, o))

    def g1_copy(part, o):
        ref = all_ref.at[me, :, lanes[part]]
        return remote(ref, ref, sems(g1_sem, part, o), gx.device(part, o, 0))

    def g2_copy(part, o):
        whole = all_ref.reshape(side, side, 2, per, 2 * hd)
        ref = whole.at[gx.cy, :, core, :, lanes[0]] if part == 0 else whole.at[:, gx.cx, core, :, lanes[1]]
        return remote(ref, ref, sems(g2_sem, part, o), gx.device(part, 0, o))

    def each(make, act):
        for part in (0, 1):
            for o in range(1, side):
                getattr(make(part, o), act)()

    def q_copy(o):
        return remote(dq_ref.at[lax.rem(chip + o, nc)], dqa_ref.at[chip], (q_sem.at[0, o], q_sem.at[1, o]), peer(o))

    each(r1_copy, "start")
    gw.second()

    def over_blocks(src_ref, work, pump):
        def load(j):
            slot = lax.rem(j, 2)
            return [pltpu.make_async_copy(
                src_ref.at[pl.ds(4 * j + 2 * u, 2)], buf.at[slot, pl.ds(2 * u, 2)], b_sem.at[slot, u]) for u in (0, 1)]

        for cp in load(0):
            cp.start()

        @pl.loop(0, nb)
        def _(j):
            for cp in load(j):
                cp.wait()

            @pl.when(j + 1 < nb)
            def _():
                for cp in load(j + 1):
                    cp.start()

            for at, ks in pump.items():
                @pl.when(j == at)
                def _():
                    for k in ks:
                        gw.third(k)

            @pl.loop(0, nb)
            def _(c):
                cols = pl.ds(pl.multiple_of(c * BLK, BLK), BLK)
                work(j, c, cols, buf[lax.rem(j, 2), :, :, :, cols].reshape(BLK, BLK))

    def out_grad(j, c, at, block):
        dwo_ref[:, at] += _dot(ot_ref[j], block)

    def query_grad(j, c, at, block):
        s_ref[c, 3 * hd : 4 * hd] += _dot(dqt_ref[j], block)

    s_ref[:, 3 * hd : 4 * hd] = jnp.zeros((nb, hd, BLK), F32)
    s_ref[:, 0:rows] = jnp.zeros((nb, rows, BLK), F32)
    over_blocks(dyf_ref, out_grad, {0: (2, 3), 3: (4, 5)})
    out_store = pltpu.make_async_copy(dwo_ref, dwo_out, o_sem.at[0])
    out_store.start()
    each(r1_copy, "wait")
    for z in range(side):
        for part in (0, 1):
            got = psum[z, gx.cx, :, 0:hd] if part == 0 else psum[gx.cy, z, :, hd:]
            for o in range(1, side):
                got = got + r1_ref[part, o, z]
            acc_ref[part, z] = got
    each(r2_copy, "start")

    @pl.loop(1, nc)
    def _(o):
        q_copy(o).start()

    over_blocks(xf_ref, query_grad, {2: (6, 7)})
    each(r2_copy, "wait")
    for part in (0, 1):
        got = acc_ref[part, here[1 - part]]
        for o in range(1, side):
            got = got + r2_ref[part, o]
        all_ref[me, :, part * hd : (part + 1) * hd] = got.astype(BF16)
    each(g1_copy, "start")
    gx.finish()
    gy.finish()

    @pl.loop(0, nb)
    def _(c):
        dwq_ref[pl.ds(pl.multiple_of(c * BLK, BLK), BLK), :] = jnp.transpose(s_ref[c, 3 * hd : 4 * hd])

    query_store = pltpu.make_async_copy(dwq_ref, dwq_out, o_sem.at[1])
    query_store.start()

    @pl.loop(1, nc)
    def _(o):
        q_copy(o).wait()

    both = (((1,), (1,)), ((), ()))

    def chip_of(k):
        return jnp.where(k < 9, near(k), far(k - 9))

    def add_heads(z):
        a = jnp.concatenate([dqa_ref[chip_of(2 * z)], dqa_ref[chip_of(2 * z + 1)]], axis=1)

        @pl.loop(0, nb)
        def _(c):
            here = pl.ds(pl.multiple_of(c * BLK, BLK), BLK)
            slot = lax.rem(z, 2)
            w = jnp.concatenate([wbuf[slot, 0, here, :], wbuf[slot, 1, here, :]], axis=1)
            s_ref[c, 0:rows] += lax.dot_general(a, w, both, preferred_element_type=F32)

    def load_heads(z):
        return [pltpu.make_async_copy(
            wqf_ref.at[2 * chip_of(2 * z + u) + core], wbuf.at[lax.rem(z, 2), u].reshape(wq_ref.shape),
            b_sem.at[lax.rem(z, 2), u]) for u in (0, 1)]

    gw.near_ready()
    for cp in load_heads(0):
        cp.start()

    def over_heads(lo, hi, hook=None):
        @pl.loop(lo, hi)
        def _(z):
            for cp in load_heads(z):
                cp.wait()

            @pl.when(z + 1 < hi)
            def _():
                for cp in load_heads(z + 1):
                    cp.start()

            add_heads(z)
            if hook is not None:
                @pl.when(z == lo + 1)
                def _():
                    hook()

    def spread():
        each(g1_copy, "wait")
        each(g2_copy, "start")

    over_heads(0, 4, spread)
    for f in range(3):
        gw.last(f)
    for cp in load_heads(4):
        cp.start()
    over_heads(4, 7)
    each(g2_copy, "wait")
    pairs = all_ref.reshape(nc, 2, per, 2 * hd)
    hand_all = remote(pairs.at[:, core], pairs.at[:, core], (f_sem.at[0], f_sem.at[1]), partner)
    hand_all.start()
    gw.last(3)
    for cp in load_heads(7):
        cp.start()
    over_heads(7, 8)
    swap = remote(s_ref.at[:, pl.ds(pl.multiple_of((1 - core) * per, per), per)], s_ref.at[:, pl.ds(rows, per)],
                  (a_sem.at[0], a_sem.at[1]), partner)
    swap.start()
    hand_all.wait()
    own_cols.wait()

    def key_grad(j, acc):
        xt = _flip(xc_ref[pl.ds(4 * j, 4)].reshape(BLK, d // n)).astype(BF16)
        return acc + _dot(xt, all_ref[pl.ds(4 * j, 4)].reshape(BLK, 2 * hd))

    r = lax.fori_loop(0, nb, key_grad, jnp.zeros((d // n, 2 * hd), F32))
    dwk_ref[...] = r[:, :hd]
    dwv_ref[...] = r[:, hd:]
    swap.wait()
    mine = all_ref[me]

    @pl.loop(0, nb)
    def _(c):
        here = pl.ds(pl.multiple_of(c * BLK, BLK), BLK)
        r = lax.dot_general(mine, w3_ref[here, hd:], both, preferred_element_type=F32)
        at = pl.ds(pl.multiple_of(core * per, per), per)
        dx_ref[:, here] = (s_ref[c, at] + s_ref[c, rows : rows + per] + r).astype(BF16)

    gw.finish()
    out_store.wait()
    query_store.wait()


def _step(x, dy, wq, wk, wv, wo, n, scale):
    rows, d = x.shape
    hd = wo.shape[0]
    t = n * rows
    nb = t // BLK
    nc = n // 2
    assert nb == 8 and 4 * rows == BLK
    nm = 2 * len(_torus_messages())
    hbm = pl.BlockSpec(memory_space=pltpu.HBM)
    vmem = pl.BlockSpec(memory_space=pltpu.VMEM)
    dma = pltpu.SemaphoreType.DMA
    full = jax.ShapeDtypeStruct((n, 4, rows // 4, d), BF16)
    head = pltpu.VMEM((t, hd), BF16)
    flat = pltpu.VMEM((nb, hd, BLK), BF16)
    return pl.pallas_call(
        functools.partial(_step_kernel, n, scale),
        in_specs=[hbm] * 6,
        out_specs=[hbm] * 3 + [vmem, hbm, vmem, vmem, hbm],
        out_shape=[
            full, full, jax.ShapeDtypeStruct((n, 4, d // 4, hd), BF16),
            jax.ShapeDtypeStruct((rows, d), BF16), jax.ShapeDtypeStruct((d, hd), F32),
            jax.ShapeDtypeStruct((d // n, hd), F32), jax.ShapeDtypeStruct((d // n, hd), F32),
            jax.ShapeDtypeStruct((hd, d), F32)],
        scratch_shapes=[
            pltpu.VMEM((d, 3 * hd), BF16), pltpu.VMEM((hd, d), BF16), head, head, head, flat, flat, flat,
            pltpu.VMEM((nb, 8, BLK), F32), head, pltpu.VMEM((nc, 2 * rows, hd), BF16), flat,
            pltpu.VMEM((nb, BLK, BLK), F32),
            pltpu.VMEM((2, 4, 4, rows // 4, d), BF16),
            pltpu.VMEM((2, 2, d, hd), BF16),
            pltpu.VMEM((nc, 2, rows, 2 * hd), F32),
            pltpu.VMEM((nc, rows, 2 * hd), F32),
            pltpu.VMEM((2, 4, 4, rows, hd), F32), pltpu.VMEM((2, 4, rows, hd), F32), pltpu.VMEM((2, 4, rows, hd), F32),
            pltpu.VMEM((n, rows, 2 * hd), BF16),
            pltpu.VMEM((nc, 2 * rows, hd), BF16),
            pltpu.VMEM((n, 4, rows // 4, d // n), BF16),
            pltpu.VMEM((d, hd), F32), pltpu.VMEM((hd, d), F32),
            dma, dma((2, nm)), dma((2, nm)), dma((2,)),
            dma, dma((2, nm)), dma((2, nm)), dma((2,)),
            dma, dma((2, nm)),
            dma((2, 2)), dma((4,)), dma, dma((2,)), dma((2, nc)), *[dma((2, 2, 4))] * 4, dma((2,)), dma((2,)), dma((2,)),
        ],
        compiler_params=pltpu.CompilerParams(collective_id=0, has_side_effects=True, vmem_limit_bytes=67043328),
        cost_estimate=pl.CostEstimate(flops=10**11, bytes_accessed=6 * t * d, transcendentals=t * t),
        name="mqa_backward",
    )(x.reshape(4, rows // 4, d), dy.reshape(4, rows // 4, d), wq.reshape(4, d // 4, hd), wk, wv, wo)


def solution(mesh):
    tok_spec = P(("data", "model"), None)
    n = mesh.shape["model"]

    def local_step(x_loc, dy_loc, wq_loc, w_key, w_value, wo_loc):
        d, hd = w_key.shape
        scale = 1.0 / math.sqrt(hd)
        _, _, _, dx, dwq, dwk, dwv, dwo = _step(
            x_loc, dy_loc, wq_loc.reshape(d, hd), w_key, w_value, wo_loc.reshape(hd, d), n, scale)
        return (dx, dwq[:, None, :], dwk, dwv, dwo[None])

    return jax.shard_map(
        local_step, mesh=mesh,
        in_specs=(tok_spec, tok_spec, P(None, "model", None), P(None, None), P(None, None), P("model", None, None)),
        out_specs=(tok_spec, P("data", "model", None), tok_spec, tok_spec, P(("data", "model"), None, None)),
        check_vma=False)
```
